1024 devices in a mesh: row: 32 (over z_hi, x, core), col: 32 (over z_lo, y).
Axes of the slice: x: 4, y: 8, z: 16 (z_hi: 4, z_lo: 4; z = z_hi * 4 + z_lo), core: 2. Of those that a mesh axis runs over, the one named last changes fastest.
Arguments:
- pressure_rhs: bfloat16 [384, 256, 384], P('col', 'row'), may hold values from -10 to 10, as said below
- scalar_source: bfloat16 [384, 256, 384], P('col', 'row'), may hold values from -10 to 10, as said below
- forward_y: bfloat16 [256, 256], replicated, may hold values from -0.375 to 0.375
- back_y: bfloat16 [256, 256], replicated, may hold values from -0.375 to 0.375
- wall_rates: float32 [256], replicated, may hold values from 0.05 to 4
Outputs:
- pressure: bfloat16 [384, 256, 384], P('col', 'row')
- scalar: bfloat16 [384, 256, 384], P('col', 'row')
The draws below stay inside these ranges and needn't reach their ends.
Inputs may be any that keep to these rules, and one draw needn't show every extreme that they name: `pressure_rhs`: a real field of order one. `scalar_source`: a real field of order one.
All inputs are finite; a program needn't handle non-finite values.
Results may differ from the reference program's by a relative error of at most 0.012.
Values may be sent and summed in bfloat16 or wider, within the bound.
No kernel may reach another device: no remote copies, remote signals or barrier semaphores. Data moves between devices by JAX's collectives and lax.ppermute only.
A program may use at most 32 MiB of HBM per device.

```python
import math
import jax
import jax.numpy as jnp
from jax import lax

NX = 384
NY = 256
NZ = 384
KEEP = 256


def rough_field(key):
    return jax.random.truncated_normal(key, -4.0, 4.0, (NZ, NY, NX), jnp.float32).astype(jnp.bfloat16)


def draw_pressure_rhs(key, part):
    return rough_field(jax.random.fold_in(key, 11))


def draw_scalar_source(key, part):
    return rough_field(jax.random.fold_in(key, 23))


def bell_draw(rng, dims, deviation, bound, kind=jnp.bfloat16):
    entries = jax.random.normal(rng, dims, jnp.float32) * deviation
    return jnp.minimum(jnp.maximum(entries, -bound), bound).astype(kind)


def setup_inputs(seed: int = 0) -> dict:
    splits = jax.random.split(jax.random.key(seed), 6)
    return {
        "pressure_rhs": draw_pressure_rhs(jax.random.fold_in(splits[5], 71), 0),
        "scalar_source": draw_scalar_source(jax.random.fold_in(splits[5], 71), 0),
        "forward_y": bell_draw(splits[2], (NY, NY), NY ** -0.5, 0.375),
        "back_y": bell_draw(splits[3], (NY, NY), NY ** -0.5, 0.375),
        "wall_rates": jnp.clip(jnp.exp(jax.random.uniform(splits[4], (NY,), jnp.float32, math.log(0.05), math.log(4.0))), 0.05, 4.0),
    }


diffusion = 0.5

def x_table(width, groups):
    half = width // 2
    per = half // groups
    column = lax.broadcasted_iota(jnp.int32, (width, width), 1)
    place = lax.broadcasted_iota(jnp.int32, (width, width), 0)
    owner = column // (2 * per)
    part = column // per % 2
    mode = owner * per + column % per
    phase = mode * place % width
    angle = phase.astype(jnp.float32) * (2.0 * math.pi / width)
    factor = math.sqrt(2.0 / width)
    return jnp.where(part == 0, factor * jnp.cos(angle), -factor * jnp.sin(angle)).astype(jnp.bfloat16)

def x_back_table(width, groups):
    half = width // 2
    per = half // groups
    line = lax.broadcasted_iota(jnp.int32, (width, width), 0)
    place = lax.broadcasted_iota(jnp.int32, (width, width), 1)
    owner = line // (2 * per)
    part = line // per % 2
    mode = owner * per + line % per
    phase = mode * place % width
    angle = phase.astype(jnp.float32) * (2.0 * math.pi / width)
    weight = jnp.where(mode == 0, 0.5, 1.0) * math.sqrt(2.0 / width)
    return jnp.where(part == 0, weight * jnp.cos(angle), -weight * jnp.sin(angle)).astype(jnp.bfloat16)

def z_tables(wave, length):
    place = lax.iota(jnp.int32, length)
    phase = wave[:, None] * place[None, :] % length
    angle = phase.astype(jnp.float32) * (2.0 * math.pi / length)
    factor = 1.0 / math.sqrt(length)
    return ((factor * jnp.cos(angle)).astype(jnp.bfloat16), (factor * jnp.sin(angle)).astype(jnp.bfloat16))

def solve_field(field, is_scalar, table_x, back_x, cosz, sinz, forward_y, back_y, wall_rates, wave):
    depth, height, width = field.shape
    half = width // 2
    kept = wave.shape[0]
    spectra = jnp.dot(field.astype(jnp.float32).reshape(depth * height, width), table_x.astype(jnp.float32))
    spectra = spectra.astype(jnp.bfloat16).astype(jnp.float32).reshape(depth, height * width)
    first = jnp.dot(cosz.astype(jnp.float32), spectra).reshape(kept, height, 2, half)
    second = jnp.dot(sinz.astype(jnp.float32), spectra).reshape(kept, height, 2, half)
    modes = jnp.stack((first[:, :, 0] + second[:, :, 1], first[:, :, 1] - second[:, :, 0]), axis=2)
    modes = modes.astype(jnp.bfloat16).astype(jnp.float32)
    coeffs = jnp.einsum('jy,kypm->kjpm', forward_y.astype(jnp.float32), modes)
    kx_sq = (lax.iota(jnp.int32, half).astype(jnp.float32) * (2.0 * math.pi / width)) ** 2
    signed = jnp.where(wave < depth // 2, wave, wave - depth)
    kz_sq = (signed.astype(jnp.float32) * (2.0 * math.pi / depth)) ** 2
    wave_sq = kz_sq[:, None] + kx_sq[None, :]
    total = wave_sq[:, None, :] + wall_rates[None, :, None]
    if is_scalar:
        hat = coeffs / (1.0 + diffusion * total)[:, :, None, :]
    else:
        hat = coeffs / (-total)[:, :, None, :]
    hat = hat.astype(jnp.bfloat16).astype(jnp.float32)
    back = jnp.einsum('yj,kjpm->kypm', back_y.astype(jnp.float32), hat)
    back = back.astype(jnp.bfloat16).astype(jnp.float32).reshape(kept, height * width)
    first = jnp.dot(cosz.astype(jnp.float32).T, back).reshape(depth, height, 2, half)
    second = jnp.dot(sinz.astype(jnp.float32).T, back).reshape(depth, height, 2, half)
    lines = jnp.stack((first[:, :, 0] - second[:, :, 1], first[:, :, 1] + second[:, :, 0]), axis=2)
    lines = lines.astype(jnp.bfloat16).astype(jnp.float32).reshape(depth * height, width)
    result = jnp.dot(lines, back_x.astype(jnp.float32))
    return result.astype(jnp.bfloat16).reshape(depth, height, width)

def reference(pressure_rhs, scalar_source, forward_y, back_y, wall_rates):
    table_x = x_table(NX, 1)
    back_x = x_back_table(NX, 1)
    wave = lax.iota(jnp.int32, KEEP)
    wave = jnp.where(wave < KEEP // 2, wave, wave + (NZ - KEEP)).astype(jnp.int32)
    cosz, sinz = z_tables(wave, NZ)
    pressure = solve_field(pressure_rhs, False, table_x, back_x, cosz, sinz, forward_y, back_y, wall_rates, wave)
    scalar = solve_field(scalar_source, True, table_x, back_x, cosz, sinz, forward_y, back_y, wall_rates, wave)
    return (pressure, scalar)
```

```python
import math

import jax
import jax.numpy as jnp
import numpy as np
from jax import lax
from jax.experimental import pallas as pl
from jax.experimental.pallas import tpu as pltpu
from jax.sharding import PartitionSpec as P

NX = 384
NY = 256
NZ = 384
KEEP = 256
DIFFUSION = 0.5
G = 32
ZL = NZ // G
YL = NY // G
PER = NX // 2 // G
ITEMS = 2 * PER
WAVES = KEEP // G
LANES = 128
BF = jnp.bfloat16
F32 = jnp.float32

KEPT = np.array([t for t in range(NZ // G) if G * t < KEEP // 2 or G * t >= NZ - KEEP // 2])


def pairs(part_out, part_in, cos, sin, sign):
    if part_out == part_in:
        return cos
    return sign * sin if part_out == 1 else -sign * sin


def items():
    for i in range(ITEMS):
        yield i // 8, i % 8, i // PER, i % PER


def x_tables():
    fwd = np.zeros((2, G, 8, NX))
    back = np.zeros((2, G, 8, NX))
    x = np.arange(NX)
    factor = math.sqrt(2.0 / NX)
    for h, i, p, k in items():
        m = np.arange(G)[:, None] * PER + k
        angle = 2.0 * math.pi * (m * x[None, :] % NX) / NX
        value = factor * (np.cos(angle) if p == 0 else -np.sin(angle))
        fwd[h, :, i] = value
        back[h, :, i] = np.where(m == 0, 0.5, 1.0) * value
    return fwd.reshape(-1, NX), back.reshape(-1, NX)


def z_outer(sign):
    out = np.zeros((2, G, 8, 2, G, 8))
    angle = 2.0 * math.pi * (np.outer(np.arange(G), np.arange(G)) % G) / G
    cos, sin = np.cos(angle) / math.sqrt(G), np.sin(angle) / math.sqrt(G)
    for h, i, p, k in items():
        for q in range(2):
            out[q, :, k, h, :, i] = pairs(q, p, cos, sin, sign)
    return out.reshape(2 * G * 8, 2 * G * 8)


def z_outer_back():
    out = np.zeros((2, G, 8, 2, G, 8))
    angle = 2.0 * math.pi * (np.outer(np.arange(G), np.arange(G)) % G) / G
    cos, sin = np.cos(angle) / math.sqrt(G), np.sin(angle) / math.sqrt(G)
    for h, i, p, k in items():
        for q in range(2):
            out[h, :, i, q, :, k] = pairs(p, q, cos, sin, 1)
    return out.reshape(2 * G * 8, 2 * G * 8)


def z_inner(sign):
    out = np.zeros((2, WAVES, YL, 2, LANES))
    angle = 2.0 * math.pi * (np.outer(KEPT, np.arange(ZL)) % ZL) / ZL
    cos, sin = np.cos(angle) / math.sqrt(ZL), np.sin(angle) / math.sqrt(ZL)
    for a in range(2):
        for b in range(2):
            w = pairs(a, b, cos, sin, -1) if sign < 0 else pairs(b, a, cos, sin, 1)
            for y in range(YL):
                out[a, :, y, b, y : ZL * YL : YL] = w
    return out.reshape(2 * WAVES * YL, 2 * LANES)


def twiddles():
    angle = 2.0 * math.pi * np.outer(np.arange(G), np.arange(ZL)) / NZ
    angle = np.repeat(np.repeat(angle, 8, axis=0), YL, axis=1)
    pad = LANES - ZL * YL
    return np.pad(np.cos(angle), ((0, 0), (0, pad))), np.pad(np.sin(angle), ((0, 0), (0, pad)))


def dot(a, b, ca=1, cb=0):
    return lax.dot_general(a, b, (((ca,), (cb,)), ((), ())), preferred_element_type=F32)


def pack(g, roll):
    n = G * 8
    mid = g[n:, :LANES] + roll(g[n:, LANES:], 4, 0)
    tiles = [v.reshape(G, 8, LANES) for v in (g[:n, :LANES], mid, g[:n, LANES:])]
    return jnp.concatenate(tiles, axis=1).reshape(G * 24, LANES).astype(BF)


def unpack(x, roll):
    n = G * 8
    x = x.astype(F32).reshape(G, 24, LANES)
    first, mid, last = (x[:, 8 * j : 8 * j + 8].reshape(n, LANES) for j in range(3))
    return (
        jnp.concatenate((first, mid), axis=0).astype(BF),
        jnp.concatenate((last, roll(mid, n - 4, 0)), axis=0).astype(BF),
    )


def swap_blocks(rows, roll):
    lane = lax.broadcasted_iota(jnp.int32, (8, LANES), 1) // 8
    x = list(rows)
    for d in (8, 4, 2, 1):
        high = (lane & d) != 0
        for i in range(16):
            if not i & d:
                a, b = x[i], x[i + d]
                x[i] = jnp.where(high, roll(b, 8 * d, 1), a)
                x[i + d] = jnp.where(high, b, roll(a, LANES - 8 * d, 1))
    return x


def stage1(p, s, table, roll):
    zero = jnp.zeros((LANES - ZL * YL, NX), BF)
    both = jnp.concatenate((p, zero, s, zero), axis=0)
    return pack(dot(table, both, 1, 1), roll)


def stage2(x, outer, inner, cw, sw, roll):
    n = G * 8
    g = dot(outer, jnp.concatenate(unpack(x, roll), axis=1))
    cols = []
    for f in range(2):
        re, im = (g[j * n : (j + 1) * n, f * LANES : (f + 1) * LANES] for j in range(2))
        h = jnp.concatenate((re * cw + im * sw, im * cw - re * sw), axis=1).astype(BF)
        o = dot(inner, h, 1, 1)
        rows = []
        for q in range(2):
            rows += swap_blocks([o[8 * i : 8 * i + 8, q * LANES : (q + 1) * LANES] for i in range(16)], roll)
        cols.append(jnp.concatenate(rows, axis=0))
    return jnp.concatenate(cols, axis=1).astype(BF)


def stage3(x, forward_y, back_y, total):
    c = dot(forward_y, x)
    hat = jnp.concatenate(
        (c[:, :LANES] / (-total), c[:, LANES:] / (1.0 + DIFFUSION * total)), axis=1
    ).astype(BF)
    return dot(back_y, hat).astype(BF)


def stage4(x, outer, inner, cw, sw, roll):
    x = x.astype(F32)
    parts = []
    for f in range(2):
        tiles = [x[8 * r : 8 * r + 8, f * LANES : (f + 1) * LANES] for r in range(G)]
        halves = [jnp.concatenate(swap_blocks(tiles[16 * q : 16 * q + 16], roll), axis=0) for q in range(2)]
        v = jnp.concatenate(halves, axis=1).astype(BF)
        h = dot(v, inner, 0, 0)
        re, im = h[:, :LANES], h[:, LANES:]
        parts.append(jnp.concatenate((re * cw - im * sw, im * cw + re * sw), axis=0).astype(BF))
    return pack(dot(outer, jnp.concatenate(parts, axis=1)), roll)


def stage5(x, table, roll):
    return tuple(dot(v, table, 0, 0)[: ZL * YL].astype(BF) for v in unpack(x, roll))


def call(fn, out, *args):
    outs = out if isinstance(out, list) else [out]
    single = outs is not out

    def kernel(*refs):
        result = fn(*(r[...] for r in refs[: len(args)]))
        for ref, value in zip(refs[len(args) :], (result,) if single else result, strict=True):
            ref[...] = value

    vmem = pl.BlockSpec(memory_space=pltpu.VMEM)
    shapes = tuple(jax.ShapeDtypeStruct(s, BF) for s in outs)
    result = pl.pallas_call(
        kernel,
        out_shape=shapes,
        in_specs=[vmem] * len(args),
        out_specs=(vmem,) * len(outs),
        name=fn.__name__,
    )(*args)
    return result[0] if single else result


def wave_numbers(row_at, col_at):
    lane = lax.iota(jnp.int32, LANES)
    k = lane % 8
    t = lane // 8 % WAVES
    m = col_at * PER + k
    n = row_at + G * t
    signed = jnp.where(t < WAVES // 2, n, n - KEEP)
    kx_sq = (m.astype(F32) * (2.0 * math.pi / NX)) ** 2
    kz_sq = (signed.astype(F32) * (2.0 * math.pi / NZ)) ** 2
    return kz_sq + kx_sq


def shards(pressure_rhs, scalar_source, forward_y, back_y, wall_rates):
    fwd_x, back_x = (jnp.asarray(t, BF) for t in x_tables())
    outer_f, outer_b = jnp.asarray(z_outer(-1), BF), jnp.asarray(z_outer_back(), BF)
    inner_f, inner_b = jnp.asarray(z_inner(-1), BF), jnp.asarray(z_inner(1), BF)
    cw, sw = (jnp.asarray(t, F32) for t in twiddles())
    total = wall_rates[:, None] + wave_numbers(lax.axis_index("row"), lax.axis_index("col"))[None, :]
    roll = pltpu.roll

    def exchange(x, axis):
        shape = x.shape
        x = x.reshape(G, -1, shape[1])
        return lax.all_to_all(x, axis, split_axis=0, concat_axis=0, tiled=True).reshape(shape)

    def s1(*a):
        return stage1(*a, roll)

    def s2(*a):
        return stage2(*a, roll)

    def s4(*a):
        return stage4(*a, roll)

    def s5(*a):
        return stage5(*a, roll)

    flat = (ZL * YL, NX)
    x = call(s1, (G * 24, LANES), pressure_rhs.reshape(flat), scalar_source.reshape(flat), fwd_x)
    x = exchange(x, "col")
    x = call(s2, (NY, 2 * LANES), x, outer_f, inner_f, cw, sw)
    x = exchange(x, "row")
    x = call(stage3, (NY, 2 * LANES), x, forward_y, back_y, total)
    x = exchange(x, "row")
    x = call(s4, (G * 24, LANES), x, outer_b, inner_b, cw, sw)
    x = exchange(x, "col")
    outs = call(s5, [flat, flat], x, back_x)
    return tuple(o.reshape(ZL, YL, NX) for o in outs)


def solution(mesh):
    field = P("col", "row", None)
    return jax.shard_map(
        shards,
        mesh=mesh,
        in_specs=(field, field, P(), P(), P()),
        out_specs=(field, field),
        check_vma=False,
    )
```

```python
import math

import jax
import jax.numpy as jnp
import numpy as np
from jax import lax
from jax.experimental import pallas as pl
from jax.experimental.pallas import tpu as pltpu
from jax.sharding import PartitionSpec as P

NX = 384
NY = 256
NZ = 384
KEEP = 256
DIFFUSION = 0.5
G = 32
ZL = NZ // G
YL = NY // G
PER = NX // 2 // G
ITEMS = 2 * PER
WAVES = KEEP // G
LANES = 128
BF = jnp.bfloat16
F32 = jnp.float32

KEPT = np.array([t for t in range(NZ // G) if G * t < KEEP // 2 or G * t >= NZ - KEEP // 2])


def pairs(part_out, part_in, cos, sin, sign):
    if part_out == part_in:
        return cos
    return sign * sin if part_out == 1 else -sign * sin


def items():
    for i in range(ITEMS):
        yield i // 8, i % 8, i // PER, i % PER


def x_tables():
    fwd = np.zeros((2, G, 8, NX))
    back = np.zeros((2, G, 8, NX))
    x = np.arange(NX)
    factor = math.sqrt(2.0 / NX)
    for h, i, p, k in items():
        m = np.arange(G)[:, None] * PER + k
        angle = 2.0 * math.pi * (m * x[None, :] % NX) / NX
        value = factor * (np.cos(angle) if p == 0 else -np.sin(angle))
        fwd[h, :, i] = value
        back[h, :, i] = np.where(m == 0, 0.5, 1.0) * value
    return fwd.reshape(-1, NX), back.reshape(-1, NX)


def z_outer(sign):
    out = np.zeros((2, G, 8, 2, G, 8))
    angle = 2.0 * math.pi * (np.outer(np.arange(G), np.arange(G)) % G) / G
    cos, sin = np.cos(angle) / math.sqrt(G), np.sin(angle) / math.sqrt(G)
    for h, i, p, k in items():
        for q in range(2):
            out[q, :, k, h, :, i] = pairs(q, p, cos, sin, sign)
    return out.reshape(2 * G * 8, 2 * G * 8)


def z_outer_back():
    out = np.zeros((2, G, 8, 2, G, 8))
    angle = 2.0 * math.pi * (np.outer(np.arange(G), np.arange(G)) % G) / G
    cos, sin = np.cos(angle) / math.sqrt(G), np.sin(angle) / math.sqrt(G)
    for h, i, p, k in items():
        for q in range(2):
            out[h, :, i, q, :, k] = pairs(p, q, cos, sin, 1)
    return out.reshape(2 * G * 8, 2 * G * 8)


def z_inner(sign):
    out = np.zeros((2, WAVES, YL, 2, LANES))
    angle = 2.0 * math.pi * (np.outer(KEPT, np.arange(ZL)) % ZL) / ZL
    cos, sin = np.cos(angle) / math.sqrt(ZL), np.sin(angle) / math.sqrt(ZL)
    for a in range(2):
        for b in range(2):
            w = pairs(a, b, cos, sin, -1) if sign < 0 else pairs(b, a, cos, sin, 1)
            for y in range(YL):
                out[a, :, y, b, y : ZL * YL : YL] = w
    return out.reshape(2 * WAVES * YL, 2 * LANES)


def twiddles():
    angle = 2.0 * math.pi * np.outer(np.arange(G), np.arange(ZL)) / NZ
    angle = np.repeat(np.repeat(angle, 8, axis=0), YL, axis=1)
    pad = LANES - ZL * YL
    return np.pad(np.cos(angle), ((0, 0), (0, pad))), np.pad(np.sin(angle), ((0, 0), (0, pad)))


def dot(a, b, ca=1, cb=0):
    return lax.dot_general(a, b, (((ca,), (cb,)), ((), ())), preferred_element_type=F32)


def pack(g, roll):
    n = G * 8
    mid = g[n:, :LANES] + roll(g[n:, LANES:], 4, 0)
    tiles = [v.reshape(G, 8, LANES) for v in (g[:n, :LANES], mid, g[:n, LANES:])]
    return jnp.concatenate(tiles, axis=1).reshape(G * 24, LANES).astype(BF)


def unpack(x, roll):
    n = G * 8
    x = x.astype(F32).reshape(G, 24, LANES)
    first, mid, last = (x[:, 8 * j : 8 * j + 8].reshape(n, LANES) for j in range(3))
    return (
        jnp.concatenate((first, mid), axis=0).astype(BF),
        jnp.concatenate((last, roll(mid, n - 4, 0)), axis=0).astype(BF),
    )


def swap_blocks(rows, roll):
    lane = lax.broadcasted_iota(jnp.int32, (8, LANES), 1) // 8
    x = list(rows)
    for d in (8, 4, 2, 1):
        high = (lane & d) != 0
        for i in range(16):
            if not i & d:
                a, b = x[i], x[i + d]
                x[i] = jnp.where(high, roll(b, 8 * d, 1), a)
                x[i + d] = jnp.where(high, b, roll(a, LANES - 8 * d, 1))
    return x


def stage1(p, s, table, roll):
    zero = jnp.zeros((LANES - ZL * YL, NX), BF)
    both = jnp.concatenate((p, zero, s, zero), axis=0)
    return pack(dot(table, both, 1, 1), roll)


def stage2(x, outer, inner, cw, sw, roll):
    n = G * 8
    g = dot(outer, jnp.concatenate(unpack(x, roll), axis=1))
    cols = []
    for f in range(2):
        re, im = (g[j * n : (j + 1) * n, f * LANES : (f + 1) * LANES] for j in range(2))
        h = jnp.concatenate((re * cw + im * sw, im * cw - re * sw), axis=1).astype(BF)
        o = dot(inner, h, 1, 1)
        rows = []
        for q in range(2):
            rows += swap_blocks([o[8 * i : 8 * i + 8, q * LANES : (q + 1) * LANES] for i in range(16)], roll)
        cols.append(jnp.concatenate(rows, axis=0))
    return jnp.concatenate(cols, axis=1).astype(BF)


def stage3(x, forward_y, back_y, total):
    c = dot(forward_y, x)
    hat = jnp.concatenate(
        (c[:, :LANES] / (-total), c[:, LANES:] / (1.0 + DIFFUSION * total)), axis=1
    ).astype(BF)
    return dot(back_y, hat).astype(BF)


def stage4(x, outer, inner, cw, sw, roll):
    x = x.astype(F32)
    parts = []
    for f in range(2):
        tiles = [x[8 * r : 8 * r + 8, f * LANES : (f + 1) * LANES] for r in range(G)]
        halves = [jnp.concatenate(swap_blocks(tiles[16 * q : 16 * q + 16], roll), axis=0) for q in range(2)]
        v = jnp.concatenate(halves, axis=1).astype(BF)
        h = dot(v, inner, 0, 0)
        re, im = h[:, :LANES], h[:, LANES:]
        parts.append(jnp.concatenate((re * cw - im * sw, im * cw + re * sw), axis=0).astype(BF))
    return pack(dot(outer, jnp.concatenate(parts, axis=1)), roll)


def stage5(x, table, roll):
    return tuple(dot(v, table, 0, 0)[: ZL * YL].astype(BF) for v in unpack(x, roll))


def call(fn, out, *args, fast=(True, True)):
    outs = out if isinstance(out, list) else [out]
    single = outs is not out

    def kernel(*refs):
        result = fn(*(r[...] for r in refs[: len(args)]))
        for ref, value in zip(refs[len(args) :], (result,) if single else result, strict=True):
            ref[...] = value

    vmem = pl.BlockSpec(memory_space=pltpu.VMEM)
    make = pltpu.VMEM if fast[1] else jax.ShapeDtypeStruct
    shapes = tuple(make(s, BF) for s in outs)
    if fast[0]:
        args = [pltpu.with_memory_space_constraint(a, pltpu.VMEM) for a in args]
    result = pl.pallas_call(
        kernel,
        out_shape=shapes,
        in_specs=[vmem] * len(args),
        out_specs=(vmem,) * len(outs),
        name=fn.__name__,
    )(*args)
    return result[0] if single else result


def wave_numbers(row_at, col_at):
    lane = lax.iota(jnp.int32, LANES)
    k = lane % 8
    t = lane // 8 % WAVES
    m = col_at * PER + k
    n = row_at + G * t
    signed = jnp.where(t < WAVES // 2, n, n - KEEP)
    kx_sq = (m.astype(F32) * (2.0 * math.pi / NX)) ** 2
    kz_sq = (signed.astype(F32) * (2.0 * math.pi / NZ)) ** 2
    return kz_sq + kx_sq


def shards(pressure_rhs, scalar_source, forward_y, back_y, wall_rates):
    fwd_x, back_x = (jnp.asarray(t, BF) for t in x_tables())
    outer_f, outer_b = jnp.asarray(z_outer(-1), BF), jnp.asarray(z_outer_back(), BF)
    inner_f, inner_b = jnp.asarray(z_inner(-1), BF), jnp.asarray(z_inner(1), BF)
    cw, sw = (jnp.asarray(t, F32) for t in twiddles())
    total = wall_rates[:, None] + wave_numbers(lax.axis_index("row"), lax.axis_index("col"))[None, :]
    roll = pltpu.roll

    def exchange(x, axis):
        shape = x.shape
        x = x.reshape(G, -1, shape[1])
        return lax.all_to_all(x, axis, split_axis=0, concat_axis=0, tiled=True).reshape(shape)

    def s1(*a):
        return stage1(*a, roll)

    def s2(*a):
        return stage2(*a, roll)

    def s4(*a):
        return stage4(*a, roll)

    def s5(*a):
        return stage5(*a, roll)

    flat = (ZL * YL, NX)
    x = call(s1, (G * 24, LANES), pressure_rhs.reshape(flat), scalar_source.reshape(flat), fwd_x, fast=(False, True))
    x = exchange(x, "col")
    x = call(s2, (NY, 2 * LANES), x, outer_f, inner_f, cw, sw)
    x, total = lax.optimization_barrier((x, total))
    x = exchange(x, "row")
    x = call(stage3, (NY, 2 * LANES), x, forward_y, back_y, total)
    x = exchange(x, "row")
    x = call(s4, (G * 24, LANES), x, outer_b, inner_b, cw, sw)
    x = exchange(x, "col")
    outs = call(s5, [flat, flat], x, back_x, fast=(True, False))
    return tuple(o.reshape(ZL, YL, NX) for o in outs)


def solution(mesh):
    field = P("col", "row", None)
    return jax.shard_map(
        shards,
        mesh=mesh,
        in_specs=(field, field, P(), P(), P()),
        out_specs=(field, field),
        check_vma=False,
    )
```

```python
import math

import jax
import jax.numpy as jnp
import numpy as np
from jax import lax
from jax.experimental import pallas as pl
from jax.experimental.pallas import tpu as pltpu
from jax.sharding import PartitionSpec as P

NX = 384
NY = 256
NZ = 384
KEEP = 256
DIFFUSION = 0.5
G = 32
ZL = NZ // G
YL = NY // G
PER = NX // 2 // G
ITEMS = 2 * PER
WAVES = KEEP // G
LANES = 128
BF = jnp.bfloat16
F32 = jnp.float32

KEPT = np.array([t for t in range(NZ // G) if G * t < KEEP // 2 or G * t >= NZ - KEEP // 2])


def pairs(part_out, part_in, cos, sin, sign):
    if part_out == part_in:
        return cos
    return sign * sin if part_out == 1 else -sign * sin


def items():
    for i in range(ITEMS):
        yield i // 8, i % 8, i // PER, i % PER


def x_tables():
    fwd = np.zeros((2, G, 8, NX))
    back = np.zeros((2, G, 8, NX))
    x = np.arange(NX)
    factor = math.sqrt(2.0 / NX)
    for h, i, p, k in items():
        m = np.arange(G)[:, None] * PER + k
        angle = 2.0 * math.pi * (m * x[None, :] % NX) / NX
        value = factor * (np.cos(angle) if p == 0 else -np.sin(angle))
        fwd[h, :, i] = value
        back[h, :, i] = np.where(m == 0, 0.5, 1.0) * value
    return fwd.reshape(-1, NX), back.reshape(-1, NX)


def z_outer(sign):
    out = np.zeros((2, G, 8, 2, G, 8))
    angle = 2.0 * math.pi * (np.outer(np.arange(G), np.arange(G)) % G) / G
    cos, sin = np.cos(angle) / math.sqrt(G), np.sin(angle) / math.sqrt(G)
    for h, i, p, k in items():
        for q in range(2):
            out[q, :, k, h, :, i] = pairs(q, p, cos, sin, sign)
    return out.reshape(2 * G * 8, 2 * G * 8)


def z_outer_back():
    out = np.zeros((2, G, 8, 2, G, 8))
    angle = 2.0 * math.pi * (np.outer(np.arange(G), np.arange(G)) % G) / G
    cos, sin = np.cos(angle) / math.sqrt(G), np.sin(angle) / math.sqrt(G)
    for h, i, p, k in items():
        for q in range(2):
            out[h, :, i, q, :, k] = pairs(p, q, cos, sin, 1)
    return out.reshape(2 * G * 8, 2 * G * 8)


def z_inner(sign):
    out = np.zeros((2, WAVES, YL, 2, LANES))
    angle = 2.0 * math.pi * (np.outer(KEPT, np.arange(ZL)) % ZL) / ZL
    cos, sin = np.cos(angle) / math.sqrt(ZL), np.sin(angle) / math.sqrt(ZL)
    for a in range(2):
        for b in range(2):
            w = pairs(a, b, cos, sin, -1) if sign < 0 else pairs(b, a, cos, sin, 1)
            for y in range(YL):
                out[a, :, y, b, y : ZL * YL : YL] = w
    return out.reshape(2 * WAVES * YL, 2 * LANES)


def twiddles():
    angle = 2.0 * math.pi * np.outer(np.arange(G), np.arange(ZL)) / NZ
    angle = np.repeat(np.repeat(angle, 8, axis=0), YL, axis=1)
    pad = LANES - ZL * YL
    return np.pad(np.cos(angle), ((0, 0), (0, pad))), np.pad(np.sin(angle), ((0, 0), (0, pad)))


def dot(a, b, ca=1, cb=0):
    return lax.dot_general(a, b, (((ca,), (cb,)), ((), ())), preferred_element_type=F32)


def pack(g, roll):
    n = G * 8
    mid = g[n:, :LANES] + roll(g[n:, LANES:], 4, 0)
    tiles = [v.reshape(G, 8, LANES) for v in (g[:n, :LANES], mid, g[:n, LANES:])]
    return jnp.concatenate(tiles, axis=1).reshape(G * 24, LANES).astype(BF)


def unpack(x, roll):
    n = G * 8
    x = x.astype(F32).reshape(G, 24, LANES)
    first, mid, last = (x[:, 8 * j : 8 * j + 8].reshape(n, LANES) for j in range(3))
    return (
        jnp.concatenate((first, mid), axis=0).astype(BF),
        jnp.concatenate((last, roll(mid, n - 4, 0)), axis=0).astype(BF),
    )


def swap_blocks(rows, roll):
    lane = lax.broadcasted_iota(jnp.int32, (8, LANES), 1) // 8
    x = list(rows)
    for d in (8, 4, 2, 1):
        high = (lane & d) != 0
        for i in range(16):
            if not i & d:
                a, b = x[i], x[i + d]
                x[i] = jnp.where(high, roll(b, 8 * d, 1), a)
                x[i + d] = jnp.where(high, b, roll(a, LANES - 8 * d, 1))
    return x


def stage1(p, s, table, roll):
    zero = jnp.zeros((LANES - ZL * YL, NX), BF)
    both = jnp.concatenate((p, zero, s, zero), axis=0)
    return pack(dot(table, both, 1, 1), roll)


def stage2(x, outer, inner, cw, sw, roll):
    n = G * 8
    g = dot(outer, jnp.concatenate(unpack(x, roll), axis=1))
    cols = []
    for f in range(2):
        re, im = (g[j * n : (j + 1) * n, f * LANES : (f + 1) * LANES] for j in range(2))
        h = jnp.concatenate((re * cw + im * sw, im * cw - re * sw), axis=1).astype(BF)
        o = dot(inner, h, 1, 1)
        rows = []
        for q in range(2):
            rows += swap_blocks([o[8 * i : 8 * i + 8, q * LANES : (q + 1) * LANES] for i in range(16)], roll)
        cols.append(jnp.concatenate(rows, axis=0))
    return jnp.concatenate(cols, axis=1).astype(BF)


def stage3(x, forward_y, back_y, wall, row_at, col_at):
    total = jnp.broadcast_to(wall, (LANES, NY)).T + wave_numbers(row_at, col_at)
    c = dot(forward_y, x)
    hat = jnp.concatenate(
        (c[:, :LANES] / (-total), c[:, LANES:] / (1.0 + DIFFUSION * total)), axis=1
    ).astype(BF)
    return dot(back_y, hat).astype(BF)


def stage4(x, outer, inner, cw, sw, roll):
    x = x.astype(F32)
    parts = []
    for f in range(2):
        tiles = [x[8 * r : 8 * r + 8, f * LANES : (f + 1) * LANES] for r in range(G)]
        halves = [jnp.concatenate(swap_blocks(tiles[16 * q : 16 * q + 16], roll), axis=0) for q in range(2)]
        v = jnp.concatenate(halves, axis=1).astype(BF)
        h = dot(v, inner, 0, 0)
        re, im = h[:, :LANES], h[:, LANES:]
        parts.append(jnp.concatenate((re * cw - im * sw, im * cw + re * sw), axis=0).astype(BF))
    return pack(dot(outer, jnp.concatenate(parts, axis=1)), roll)


def stage5(x, table, roll):
    return tuple(dot(v, table, 0, 0)[: ZL * YL].astype(BF) for v in unpack(x, roll))


def call(fn, out, *args, fast=(True, True)):
    outs = out if isinstance(out, list) else [out]
    single = outs is not out

    def kernel(*refs):
        result = fn(*(r[...] for r in refs[: len(args)]))
        for ref, value in zip(refs[len(args) :], (result,) if single else result, strict=True):
            ref[...] = value

    vmem = pl.BlockSpec(memory_space=pltpu.VMEM)
    make = pltpu.VMEM if fast[1] else jax.ShapeDtypeStruct
    shapes = tuple(make(s, BF) for s in outs)
    if fast[0]:
        args = [pltpu.with_memory_space_constraint(a, pltpu.VMEM) for a in args]
    result = pl.pallas_call(
        kernel,
        out_shape=shapes,
        in_specs=[vmem] * len(args),
        out_specs=(vmem,) * len(outs),
        name=fn.__name__,
    )(*args)
    return result[0] if single else result


def wave_numbers(row_at, col_at):
    lane = lax.broadcasted_iota(jnp.int32, (1, LANES), 1)
    k = lane % 8
    t = lane // 8 % WAVES
    m = col_at * PER + k
    n = row_at + G * t
    signed = jnp.where(t < WAVES // 2, n, n - KEEP)
    kx_sq = (m.astype(F32) * (2.0 * math.pi / NX)) ** 2
    kz_sq = (signed.astype(F32) * (2.0 * math.pi / NZ)) ** 2
    return kz_sq + kx_sq


def shards(pressure_rhs, scalar_source, forward_y, back_y, wall_rates):
    fwd_x, back_x = (jnp.asarray(t, BF) for t in x_tables())
    outer_f, outer_b = jnp.asarray(z_outer(-1), BF), jnp.asarray(z_outer_back(), BF)
    inner_f, inner_b = jnp.asarray(z_inner(-1), BF), jnp.asarray(z_inner(1), BF)
    cw, sw = (jnp.asarray(t, F32) for t in twiddles())
    roll = pltpu.roll

    def exchange(x, axis):
        shape = x.shape
        x = x.reshape(G, -1, shape[1])
        return lax.all_to_all(x, axis, split_axis=0, concat_axis=0, tiled=True).reshape(shape)

    def s1(*a):
        return stage1(*a, roll)

    def s2(*a):
        return stage2(*a, roll)

    def s3(*a):
        return stage3(*a, lax.axis_index("row"), lax.axis_index("col"))

    def s4(*a):
        return stage4(*a, roll)

    def s5(*a):
        return stage5(*a, roll)

    flat = (ZL * YL, NX)
    x = call(s1, (G * 24, LANES), pressure_rhs.reshape(flat), scalar_source.reshape(flat), fwd_x, fast=(False, True))
    x = exchange(x, "col")
    x = call(s2, (NY, 2 * LANES), x, outer_f, inner_f, cw, sw)
    x = exchange(x, "row")
    x = call(s3, (NY, 2 * LANES), x, forward_y, back_y, wall_rates.reshape(1, NY))
    x = exchange(x, "row")
    x = call(s4, (G * 24, LANES), x, outer_b, inner_b, cw, sw)
    x = exchange(x, "col")
    outs = call(s5, [flat, flat], x, back_x, fast=(True, False))
    return tuple(o.reshape(ZL, YL, NX) for o in outs)


def solution(mesh):
    field = P("col", "row", None)
    return jax.shard_map(
        shards,
        mesh=mesh,
        in_specs=(field, field, P(), P(), P()),
        out_specs=(field, field),
        check_vma=False,
    )
```

```python
import math

import jax
import jax.numpy as jnp
import numpy as np
from jax import lax
from jax.experimental import pallas as pl
from jax.experimental.pallas import tpu as pltpu
from jax.sharding import PartitionSpec as P

NX = 384
NY = 256
NZ = 384
KEEP = 256
DIFFUSION = 0.5
G = 32
ZL = NZ // G
YL = NY // G
PER = NX // 2 // G
ITEMS = 2 * PER
WAVES = KEEP // G
LANES = 128
BF = jnp.bfloat16
F32 = jnp.float32

KEPT = np.array([t for t in range(NZ // G) if G * t < KEEP // 2 or G * t >= NZ - KEEP // 2])


def pairs(part_out, part_in, cos, sin, sign):
    if part_out == part_in:
        return cos
    return sign * sin if part_out == 1 else -sign * sin


def items():
    for i in range(ITEMS):
        yield i // 8, i % 8, i // PER, i % PER


def x_tables():
    fwd = np.zeros((2, G, 8, NX))
    back = np.zeros((2, G, 8, NX))
    x = np.arange(NX)
    factor = math.sqrt(2.0 / NX)
    for h, i, p, k in items():
        m = np.arange(G)[:, None] * PER + k
        angle = 2.0 * math.pi * (m * x[None, :] % NX) / NX
        value = factor * (np.cos(angle) if p == 0 else -np.sin(angle))
        fwd[h, :, i] = value
        back[h, :, i] = np.where(m == 0, 0.5, 1.0) * value
    return fwd.reshape(-1, NX), back.reshape(-1, NX)


def waves(table, axis):
    shape = list(table.shape)
    shape[axis : axis + 2] = [2, G // 2 * PER]
    pad = [(0, 0)] * len(shape)
    pad[axis + 1] = (0, LANES - shape[axis + 1])
    return np.pad(table.reshape(shape), pad)


def z_outer(sign):
    out = np.zeros((2, G, PER, 2, G, 8))
    angle = 2.0 * math.pi * (np.outer(np.arange(G), np.arange(G)) % G) / G
    cos, sin = np.cos(angle) / math.sqrt(G), np.sin(angle) / math.sqrt(G)
    for h, i, p, k in items():
        for q in range(2):
            out[q, :, k, h, :, i] = pairs(q, p, cos, sin, sign)
    return waves(out, 1).reshape(4 * LANES, 2 * G * 8)


def z_outer_back():
    out = np.zeros((2, G, 8, 2, G, PER))
    angle = 2.0 * math.pi * (np.outer(np.arange(G), np.arange(G)) % G) / G
    cos, sin = np.cos(angle) / math.sqrt(G), np.sin(angle) / math.sqrt(G)
    for h, i, p, k in items():
        for q in range(2):
            out[h, :, i, q, :, k] = pairs(p, q, cos, sin, 1)
    return waves(out, 4).reshape(2 * G * 8, 4 * LANES)


def z_inner(sign):
    out = np.zeros((2, WAVES, YL, 2, LANES))
    angle = 2.0 * math.pi * (np.outer(KEPT, np.arange(ZL)) % ZL) / ZL
    cos, sin = np.cos(angle) / math.sqrt(ZL), np.sin(angle) / math.sqrt(ZL)
    for a in range(2):
        for b in range(2):
            w = pairs(a, b, cos, sin, -1) if sign < 0 else pairs(b, a, cos, sin, 1)
            for y in range(YL):
                out[a, :, y, b, y : ZL * YL : YL] = w
    return out.reshape(2 * WAVES * YL, 2 * LANES)


def twiddles():
    angle = 2.0 * math.pi * np.outer(np.arange(G), np.arange(ZL)) / NZ
    angle = np.repeat(np.repeat(angle, PER, axis=0).reshape(G, PER, ZL), YL, axis=2)
    angle = np.pad(waves(angle, 0).reshape(2 * LANES, ZL * YL), ((0, 0), (0, LANES - ZL * YL)))
    return np.cos(angle), np.sin(angle)


def dot(a, b, ca=1, cb=0):
    return lax.dot_general(a, b, (((ca,), (cb,)), ((), ())), preferred_element_type=F32)


def pack(g, roll):
    n = G * 8
    mid = g[n:, :LANES] + roll(g[n:, LANES:], 4, 0)
    tiles = [v.reshape(G, 8, LANES) for v in (g[:n, :LANES], mid, g[:n, LANES:])]
    return jnp.concatenate(tiles, axis=1).reshape(G * 24, LANES).astype(BF)


def unpack(x, roll):
    n = G * 8
    x = x.astype(F32).reshape(G, 24, LANES)
    first, mid, last = (x[:, 8 * j : 8 * j + 8].reshape(n, LANES) for j in range(3))
    return (
        jnp.concatenate((first, mid), axis=0).astype(BF),
        jnp.concatenate((last, roll(mid, n - 4, 0)), axis=0).astype(BF),
    )


def swap_blocks(rows, roll):
    lane = lax.broadcasted_iota(jnp.int32, (8, LANES), 1) // PER
    x = list(rows)
    for d in (8, 4, 2, 1):
        high = (lane & d) != 0
        for i in range(16):
            if not i & d:
                a, b = x[i], x[i + d]
                x[i] = jnp.where(high, roll(b, PER * d, 1), a)
                x[i + d] = jnp.where(high, b, roll(a, LANES - PER * d, 1))
    return x


def fold(z, roll):
    lane = lax.broadcasted_iota(jnp.int32, (NY, LANES), 1)
    moved = roll(z[1], LANES - LANES // 4, 1)
    whole = jnp.where(lane < 3 * LANES // 4, z[0], moved).reshape(G, YL, LANES)
    low = moved.reshape(G, YL, LANES)[:, :4]
    high = roll(moved, LANES // 2, 1).reshape(G, YL, LANES)[:, 4:]
    lane = lax.broadcasted_iota(jnp.int32, (G, 4, LANES), 2)
    rest = jnp.where(lane < LANES // 2, low, high)
    return jnp.concatenate((whole[:, :4], whole[:, 4:], rest), axis=2).astype(BF)


def unfold(x, roll):
    x = x.astype(F32)
    rest = x[:, :, 2 * LANES :]
    whole = jnp.concatenate((x[:, :, :LANES], x[:, :, LANES : 2 * LANES]), axis=1).reshape(NY, LANES)
    rest = jnp.concatenate((rest, roll(rest, LANES // 2, 2)), axis=1).reshape(NY, LANES)
    return whole, rest


def refold(whole, rest, roll):
    lane = lax.broadcasted_iota(jnp.int32, (G, 4, LANES), 2)
    low = rest.reshape(G, YL, LANES)[:, :4]
    high = roll(rest, LANES // 2, 1).reshape(G, YL, LANES)[:, 4:]
    whole = whole.reshape(G, YL, LANES)
    rest = jnp.where(lane < LANES // 2, low, high)
    return jnp.concatenate((whole[:, :4], whole[:, 4:], rest), axis=2).astype(BF)


def stage1(p, s, table, roll):
    zero = jnp.zeros((LANES - ZL * YL, NX), BF)
    both = jnp.concatenate((p, zero, s, zero), axis=0)
    return pack(dot(table, both, 1, 1), roll)


def stage2(x, outer, inner, cw, sw, roll):
    n = G * 8
    g = dot(outer, jnp.concatenate(unpack(x, roll), axis=1))
    cols = []
    for f in range(2):
        re, im = (g[j * n : (j + 1) * n, f * LANES : (f + 1) * LANES] for j in range(2))
        h = jnp.concatenate((re * cw + im * sw, im * cw - re * sw), axis=1).astype(BF)
        o = dot(inner, h, 1, 1)
        rows = []
        for q in range(2):
            rows += swap_blocks([o[8 * i : 8 * i + 8, q * LANES : (q + 1) * LANES] for i in range(16)], roll)
        cols.append(jnp.concatenate(rows, axis=0))
    return fold(cols, roll)


def stage3(x, forward_y, back_y, wall, row_at, col_at, roll):
    wall = jnp.broadcast_to(wall, (LANES, NY)).T
    lane = lax.broadcasted_iota(jnp.int32, (1, LANES), 1)
    c = dot(forward_y, jnp.concatenate(unfold(x, roll), axis=1).astype(BF))
    total = wall + wave_numbers(jnp.where(lane < 96, lane, lane - 96), row_at, col_at)
    scale = jnp.where(lane < 96, -total, 1.0 + DIFFUSION * total)
    rest = 1.0 + DIFFUSION * (wall + wave_numbers(lane % 64 + 32, row_at, col_at))
    hat = jnp.concatenate((c[:, :LANES] / scale, c[:, LANES:] / rest), axis=1).astype(BF)
    e = dot(back_y, hat)
    return refold(e[:, :LANES], e[:, LANES:], roll)


def stage4(x, outer, inner, cw, sw, roll):
    whole, rest = unfold(x, roll)
    lane = lax.broadcasted_iota(jnp.int32, (NY, LANES), 1)
    second = jnp.where(lane < LANES // 4, roll(whole, LANES // 4, 1), roll(rest, LANES // 4, 1))
    parts = []
    for z in (whole, second):
        tiles = [z[8 * r : 8 * r + 8] for r in range(G)]
        halves = [jnp.concatenate(swap_blocks(tiles[16 * q : 16 * q + 16], roll), axis=0) for q in range(2)]
        v = jnp.concatenate(halves, axis=1).astype(BF)
        h = dot(v, inner, 0, 0)
        re, im = h[:, :LANES], h[:, LANES:]
        parts.append(jnp.concatenate((re * cw - im * sw, im * cw + re * sw), axis=0).astype(BF))
    return pack(dot(outer, jnp.concatenate(parts, axis=1)), roll)


def stage5(x, table, roll):
    return tuple(dot(v, table, 0, 0)[: ZL * YL].astype(BF) for v in unpack(x, roll))


def call(fn, out, *args, fast=(True, True)):
    outs = out if isinstance(out, list) else [out]
    single = outs is not out

    def kernel(*refs):
        result = fn(*(r[...] for r in refs[: len(args)]))
        for ref, value in zip(refs[len(args) :], (result,) if single else result, strict=True):
            ref[...] = value

    vmem = pl.BlockSpec(memory_space=pltpu.VMEM)
    make = pltpu.VMEM if fast[1] else jax.ShapeDtypeStruct
    shapes = tuple(make(s, BF) for s in outs)
    if fast[0]:
        args = [pltpu.with_memory_space_constraint(a, pltpu.VMEM) for a in args]
    result = pl.pallas_call(
        kernel,
        out_shape=shapes,
        in_specs=[vmem] * len(args),
        out_specs=(vmem,) * len(outs),
        name=fn.__name__,
    )(*args)
    return result[0] if single else result


def wave_numbers(lane, row_at, col_at):
    k = lane % PER
    t = lane // PER % WAVES
    m = col_at * PER + k
    n = row_at + G * t
    signed = jnp.where(t < WAVES // 2, n, n - KEEP)
    kx_sq = (m.astype(F32) * (2.0 * math.pi / NX)) ** 2
    kz_sq = (signed.astype(F32) * (2.0 * math.pi / NZ)) ** 2
    return kz_sq + kx_sq


def shards(pressure_rhs, scalar_source, forward_y, back_y, wall_rates):
    fwd_x, back_x = (jnp.asarray(t, BF) for t in x_tables())
    outer_f, outer_b = jnp.asarray(z_outer(-1), BF), jnp.asarray(z_outer_back(), BF)
    inner_f, inner_b = jnp.asarray(z_inner(-1), BF), jnp.asarray(z_inner(1), BF)
    cw, sw = (jnp.asarray(t, F32) for t in twiddles())
    roll = pltpu.roll

    def exchange(x, axis):
        shape = x.shape
        x = x.reshape(G, -1, shape[-1])
        return lax.all_to_all(x, axis, split_axis=0, concat_axis=0, tiled=True).reshape(shape)

    def s1(*a):
        return stage1(*a, roll)

    def s2(*a):
        return stage2(*a, roll)

    def s3(*a):
        return stage3(*a, lax.axis_index("row"), lax.axis_index("col"), roll)

    def s4(*a):
        return stage4(*a, roll)

    def s5(*a):
        return stage5(*a, roll)

    flat = (ZL * YL, NX)
    x = call(s1, (G * 24, LANES), pressure_rhs.reshape(flat), scalar_source.reshape(flat), fwd_x, fast=(False, True))
    x = exchange(x, "col")
    x = call(s2, (G, 4, 3 * LANES), x, outer_f, inner_f, cw, sw)
    x = exchange(x, "row")
    x = call(s3, (G, 4, 3 * LANES), x, forward_y, back_y, wall_rates.reshape(1, NY))
    x = exchange(x, "row")
    x = call(s4, (G * 24, LANES), x, outer_b, inner_b, cw, sw)
    x = exchange(x, "col")
    outs = call(s5, [flat, flat], x, back_x, fast=(True, False))
    return tuple(o.reshape(ZL, YL, NX) for o in outs)


def solution(mesh):
    field = P("col", "row", None)
    return jax.shard_map(
        shards,
        mesh=mesh,
        in_specs=(field, field, P(), P(), P()),
        out_specs=(field, field),
        check_vma=False,
    )
```

```python
import math

import jax
import jax.numpy as jnp
import numpy as np
from jax import lax
from jax.experimental import pallas as pl
from jax.experimental.pallas import tpu as pltpu
from jax.sharding import PartitionSpec as P

NX = 384
NY = 256
NZ = 384
KEEP = 256
DIFFUSION = 0.5
G = 32
ZL = NZ // G
YL = NY // G
PER = NX // 2 // G
ITEMS = 2 * PER
WAVES = KEEP // G
LANES = 128
FIRST = {"row": 23, "col": 20}
BF = jnp.bfloat16
F32 = jnp.float32

KEPT = np.array([t for t in range(NZ // G) if G * t < KEEP // 2 or G * t >= NZ - KEEP // 2])


def pairs(part_out, part_in, cos, sin, sign):
    if part_out == part_in:
        return cos
    return sign * sin if part_out == 1 else -sign * sin


def items():
    for i in range(ITEMS):
        yield i // 8, i % 8, i // PER, i % PER


def x_tables():
    fwd = np.zeros((2, G, 8, NX))
    back = np.zeros((2, G, 8, NX))
    x = np.arange(NX)
    factor = math.sqrt(2.0 / NX)
    for h, i, p, k in items():
        m = np.arange(G)[:, None] * PER + k
        angle = 2.0 * math.pi * (m * x[None, :] % NX) / NX
        value = factor * (np.cos(angle) if p == 0 else -np.sin(angle))
        fwd[h, :, i] = value
        back[h, :, i] = np.where(m == 0, 0.5, 1.0) * value
    return fwd.reshape(-1, NX), back.reshape(-1, NX)


def waves(table, axis):
    shape = list(table.shape)
    shape[axis : axis + 2] = [2, G // 2 * PER]
    pad = [(0, 0)] * len(shape)
    pad[axis + 1] = (0, LANES - shape[axis + 1])
    return np.pad(table.reshape(shape), pad)


def z_outer(sign):
    out = np.zeros((2, G, PER, 2, G, 8))
    angle = 2.0 * math.pi * (np.outer(np.arange(G), np.arange(G)) % G) / G
    cos, sin = np.cos(angle) / math.sqrt(G), np.sin(angle) / math.sqrt(G)
    for h, i, p, k in items():
        for q in range(2):
            out[q, :, k, h, :, i] = pairs(q, p, cos, sin, sign)
    return waves(out, 1).reshape(4 * LANES, 2 * G * 8)


def z_outer_back():
    out = np.zeros((2, G, 8, 2, G, PER))
    angle = 2.0 * math.pi * (np.outer(np.arange(G), np.arange(G)) % G) / G
    cos, sin = np.cos(angle) / math.sqrt(G), np.sin(angle) / math.sqrt(G)
    for h, i, p, k in items():
        for q in range(2):
            out[h, :, i, q, :, k] = pairs(p, q, cos, sin, 1)
    return waves(out, 4).reshape(2 * G * 8, 4 * LANES)


def z_inner(sign):
    out = np.zeros((2, WAVES, YL, 2, LANES))
    angle = 2.0 * math.pi * (np.outer(KEPT, np.arange(ZL)) % ZL) / ZL
    cos, sin = np.cos(angle) / math.sqrt(ZL), np.sin(angle) / math.sqrt(ZL)
    for a in range(2):
        for b in range(2):
            w = pairs(a, b, cos, sin, -1) if sign < 0 else pairs(b, a, cos, sin, 1)
            for y in range(YL):
                out[a, :, y, b, y : ZL * YL : YL] = w
    return out.reshape(2 * WAVES * YL, 2 * LANES)


def twiddles():
    angle = 2.0 * math.pi * np.outer(np.arange(G), np.arange(ZL)) / NZ
    angle = np.repeat(np.repeat(angle, PER, axis=0).reshape(G, PER, ZL), YL, axis=2)
    angle = np.pad(waves(angle, 0).reshape(2 * LANES, ZL * YL), ((0, 0), (0, LANES - ZL * YL)))
    return np.cos(angle), np.sin(angle)


def dot(a, b, ca=1, cb=0):
    return lax.dot_general(a, b, (((ca,), (cb,)), ((), ())), preferred_element_type=F32)


def pack(g, roll):
    n = G * 8
    mid = g[n:, :LANES] + roll(g[n:, LANES:], 4, 0)
    tiles = [v.reshape(G, 8, LANES) for v in (g[:n, :LANES], mid, g[:n, LANES:])]
    return jnp.concatenate(tiles, axis=1).reshape(G * 24, LANES).astype(BF)


def unpack(x, roll):
    n = G * 8
    x = x.astype(F32).reshape(G, 24, LANES)
    first, mid, last = (x[:, 8 * j : 8 * j + 8].reshape(n, LANES) for j in range(3))
    return (
        jnp.concatenate((first, mid), axis=0).astype(BF),
        jnp.concatenate((last, roll(mid, n - 4, 0)), axis=0).astype(BF),
    )


def swap_blocks(rows, roll):
    lane = lax.broadcasted_iota(jnp.int32, (8, LANES), 1) // PER
    x = list(rows)
    for d in (8, 4, 2, 1):
        high = (lane & d) != 0
        for i in range(16):
            if not i & d:
                a, b = x[i], x[i + d]
                x[i] = jnp.where(high, roll(b, PER * d, 1), a)
                x[i + d] = jnp.where(high, b, roll(a, LANES - PER * d, 1))
    return x


def fold(z, roll):
    lane = lax.broadcasted_iota(jnp.int32, (NY, LANES), 1)
    moved = roll(z[1], LANES - LANES // 4, 1)
    whole = jnp.where(lane < 3 * LANES // 4, z[0], moved).reshape(G, YL, LANES)
    low = moved.reshape(G, YL, LANES)[:, :4]
    high = roll(moved, LANES // 2, 1).reshape(G, YL, LANES)[:, 4:]
    lane = lax.broadcasted_iota(jnp.int32, (G, 4, LANES), 2)
    rest = jnp.where(lane < LANES // 2, low, high)
    return jnp.concatenate((whole[:, :4], whole[:, 4:], rest), axis=2).astype(BF)


def unfold(x, roll):
    x = x.astype(F32)
    rest = x[:, :, 2 * LANES :]
    whole = jnp.concatenate((x[:, :, :LANES], x[:, :, LANES : 2 * LANES]), axis=1).reshape(NY, LANES)
    rest = jnp.concatenate((rest, roll(rest, LANES // 2, 2)), axis=1).reshape(NY, LANES)
    return whole, rest


def refold(whole, rest, roll):
    lane = lax.broadcasted_iota(jnp.int32, (G, 4, LANES), 2)
    low = rest.reshape(G, YL, LANES)[:, :4]
    high = roll(rest, LANES // 2, 1).reshape(G, YL, LANES)[:, 4:]
    whole = whole.reshape(G, YL, LANES)
    rest = jnp.where(lane < LANES // 2, low, high)
    return jnp.concatenate((whole[:, :4], whole[:, 4:], rest), axis=2).astype(BF)


def stage1(p, s, table, roll):
    zero = jnp.zeros((LANES - ZL * YL, NX), BF)
    both = jnp.concatenate((p, zero, s, zero), axis=0)
    return pack(dot(table, both, 1, 1), roll)


def stage2(x, outer, inner, cw, sw, roll):
    n = G * 8
    g = dot(outer, jnp.concatenate(unpack(x, roll), axis=1))
    cols = []
    for f in range(2):
        re, im = (g[j * n : (j + 1) * n, f * LANES : (f + 1) * LANES] for j in range(2))
        h = jnp.concatenate((re * cw + im * sw, im * cw - re * sw), axis=1).astype(BF)
        o = dot(inner, h, 1, 1)
        rows = []
        for q in range(2):
            rows += swap_blocks([o[8 * i : 8 * i + 8, q * LANES : (q + 1) * LANES] for i in range(16)], roll)
        cols.append(jnp.concatenate(rows, axis=0))
    return fold(cols, roll)


def stage3(x, forward_y, back_y, wall, row_at, col_at, roll):
    wall = jnp.broadcast_to(wall, (LANES, NY)).T
    lane = lax.broadcasted_iota(jnp.int32, (1, LANES), 1)
    c = dot(forward_y, jnp.concatenate(unfold(x, roll), axis=1).astype(BF))
    total = wall + wave_numbers(jnp.where(lane < 96, lane, lane - 96), row_at, col_at)
    scale = jnp.where(lane < 96, -total, 1.0 + DIFFUSION * total)
    rest = 1.0 + DIFFUSION * (wall + wave_numbers(lane % 64 + 32, row_at, col_at))
    hat = jnp.concatenate((c[:, :LANES] / scale, c[:, LANES:] / rest), axis=1).astype(BF)
    e = dot(back_y, hat)
    return refold(e[:, :LANES], e[:, LANES:], roll)


def stage4(x, outer, inner, cw, sw, roll):
    whole, rest = unfold(x, roll)
    lane = lax.broadcasted_iota(jnp.int32, (NY, LANES), 1)
    second = jnp.where(lane < LANES // 4, roll(whole, LANES // 4, 1), roll(rest, LANES // 4, 1))
    parts = []
    for z in (whole, second):
        tiles = [z[8 * r : 8 * r + 8] for r in range(G)]
        halves = [jnp.concatenate(swap_blocks(tiles[16 * q : 16 * q + 16], roll), axis=0) for q in range(2)]
        v = jnp.concatenate(halves, axis=1).astype(BF)
        h = dot(v, inner, 0, 0)
        re, im = h[:, :LANES], h[:, LANES:]
        parts.append(jnp.concatenate((re * cw - im * sw, im * cw + re * sw), axis=0).astype(BF))
    return pack(dot(outer, jnp.concatenate(parts, axis=1)), roll)


def stage5(x, table, roll):
    return tuple(dot(v, table, 0, 0)[: ZL * YL].astype(BF) for v in unpack(x, roll))


def turn(x, blocks):
    n = x.shape[0] // G * blocks
    return jnp.concatenate((x[n:], x[:n]), axis=0)


def call(fn, out, *args, axes=(None, None)):
    outs = out if isinstance(out, list) else [out]
    single = outs is not out

    def kernel(*refs):
        values = [r[...] for r in refs[: len(args)]]
        if axes[0]:
            values[0] = turn(values[0], G - FIRST[axes[0]])
        result = fn(*values)
        if axes[1]:
            result = turn(result, FIRST[axes[1]])
        for ref, value in zip(refs[len(args) :], (result,) if single else result, strict=True):
            ref[...] = value

    vmem = pl.BlockSpec(memory_space=pltpu.VMEM)
    make = pltpu.VMEM if axes[1] else jax.ShapeDtypeStruct
    shapes = tuple(make(s, BF) for s in outs)
    if axes[0]:
        args = [pltpu.with_memory_space_constraint(a, pltpu.VMEM) for a in args]
    result = pl.pallas_call(
        kernel,
        out_shape=shapes,
        in_specs=[vmem] * len(args),
        out_specs=(vmem,) * len(outs),
        name=fn.__name__,
    )(*args)
    return result[0] if single else result


def wave_numbers(lane, row_at, col_at):
    k = lane % PER
    t = lane // PER % WAVES
    m = col_at * PER + k
    n = row_at + G * t
    signed = jnp.where(t < WAVES // 2, n, n - KEEP)
    kx_sq = (m.astype(F32) * (2.0 * math.pi / NX)) ** 2
    kz_sq = (signed.astype(F32) * (2.0 * math.pi / NZ)) ** 2
    return kz_sq + kx_sq


def shards(pressure_rhs, scalar_source, forward_y, back_y, wall_rates):
    fwd_x, back_x = (jnp.asarray(t, BF) for t in x_tables())
    outer_f, outer_b = jnp.asarray(z_outer(-1), BF), jnp.asarray(z_outer_back(), BF)
    inner_f, inner_b = jnp.asarray(z_inner(-1), BF), jnp.asarray(z_inner(1), BF)
    cw, sw = (jnp.asarray(t, F32) for t in twiddles())
    roll = pltpu.roll

    def exchange(x, axis):
        shape = x.shape
        x = x.reshape(G, -1, shape[-1])
        group = [(i + FIRST[axis]) % G for i in range(G)]
        x = lax.all_to_all(x, axis, split_axis=0, concat_axis=0, tiled=True, axis_index_groups=[group])
        return x.reshape(shape)

    def s1(*a):
        return stage1(*a, roll)

    def s2(*a):
        return stage2(*a, roll)

    def s3(*a):
        return stage3(*a, lax.axis_index("row"), lax.axis_index("col"), roll)

    def s4(*a):
        return stage4(*a, roll)

    def s5(*a):
        return stage5(*a, roll)

    flat = (ZL * YL, NX)
    x = call(s1, (G * 24, LANES), pressure_rhs.reshape(flat), scalar_source.reshape(flat), fwd_x, axes=(None, "col"))
    x = exchange(x, "col")
    x = call(s2, (G, 4, 3 * LANES), x, outer_f, inner_f, cw, sw, axes=("col", "row"))
    x = exchange(x, "row")
    x = call(s3, (G, 4, 3 * LANES), x, forward_y, back_y, wall_rates.reshape(1, NY), axes=("row", "row"))
    x = exchange(x, "row")
    x = call(s4, (G * 24, LANES), x, outer_b, inner_b, cw, sw, axes=("row", "col"))
    x = exchange(x, "col")
    outs = call(s5, [flat, flat], x, back_x, axes=("col", None))
    return tuple(o.reshape(ZL, YL, NX) for o in outs)


def solution(mesh):
    field = P("col", "row", None)
    return jax.shard_map(
        shards,
        mesh=mesh,
        in_specs=(field, field, P(), P(), P()),
        out_specs=(field, field),
        check_vma=False,
    )
```

```python
import math

import jax
import jax.numpy as jnp
import numpy as np
from jax import lax
from jax.experimental import pallas as pl
from jax.experimental.pallas import tpu as pltpu
from jax.sharding import PartitionSpec as P

NX = 384
NY = 256
NZ = 384
KEEP = 256
DIFFUSION = 0.5
G = 32
ZL = NZ // G
YL = NY // G
PER = NX // 2 // G
ITEMS = 2 * PER
WAVES = KEEP // G
LINE = G * PER
LANES = 128
FIRST = {"row": 23, "col": 20}
BF = jnp.bfloat16
F32 = jnp.float32

KEPT = np.array([t for t in range(NZ // G) if G * t < KEEP // 2 or G * t >= NZ - KEEP // 2])


def pairs(part_out, part_in, cos, sin, sign):
    if part_out == part_in:
        return cos
    return sign * sin if part_out == 1 else -sign * sin


def items():
    for i in range(ITEMS):
        yield i // 8, i % 8, i // PER, i % PER


def x_tables():
    fwd = np.zeros((2, G, 8, NX))
    back = np.zeros((2, G, 8, NX))
    x = np.arange(NX)
    factor = math.sqrt(2.0 / NX)
    for h, i, p, k in items():
        m = np.arange(G)[:, None] * PER + k
        angle = 2.0 * math.pi * (m * x[None, :] % NX) / NX
        value = factor * (np.cos(angle) if p == 0 else -np.sin(angle))
        fwd[h, :, i] = value
        back[h, :, i] = np.where(m == 0, 0.5, 1.0) * value
    return fwd.reshape(-1, NX), back.reshape(-1, NX)


def z_outer(sign):
    out = np.zeros((2, G, PER, 2, G, 8))
    angle = 2.0 * math.pi * (np.outer(np.arange(G), np.arange(G)) % G) / G
    cos, sin = np.cos(angle) / math.sqrt(G), np.sin(angle) / math.sqrt(G)
    for h, i, p, k in items():
        for q in range(2):
            out[q, :, k, h, :, i] = pairs(q, p, cos, sin, sign)
    return out.reshape(2 * LINE, 2 * G * 8)


def z_outer_back():
    out = np.zeros((2, G, 8, 2, G, PER))
    angle = 2.0 * math.pi * (np.outer(np.arange(G), np.arange(G)) % G) / G
    cos, sin = np.cos(angle) / math.sqrt(G), np.sin(angle) / math.sqrt(G)
    for h, i, p, k in items():
        for q in range(2):
            out[h, :, i, q, :, k] = pairs(p, q, cos, sin, 1)
    return out.reshape(2 * G * 8, 2 * LINE)


def z_inner(sign):
    out = np.zeros((2, WAVES, YL, 2, LANES))
    angle = 2.0 * math.pi * (np.outer(KEPT, np.arange(ZL)) % ZL) / ZL
    cos, sin = np.cos(angle) / math.sqrt(ZL), np.sin(angle) / math.sqrt(ZL)
    for a in range(2):
        for b in range(2):
            w = pairs(a, b, cos, sin, -1) if sign < 0 else pairs(b, a, cos, sin, 1)
            for y in range(YL):
                out[a, :, y, b, y : ZL * YL : YL] = w
    return out.reshape(2 * WAVES * YL, 2 * LANES)


def twiddles():
    angle = 2.0 * math.pi * np.outer(np.arange(G), np.arange(ZL)) / NZ
    angle = np.repeat(np.repeat(angle, PER, axis=0), YL, axis=1)
    angle = np.pad(angle, ((0, 0), (0, LANES - ZL * YL)))
    return np.cos(angle), np.sin(angle)


def dot(a, b, ca=1, cb=0):
    return lax.dot_general(a, b, (((ca,), (cb,)), ((), ())), preferred_element_type=F32)


def pack(g, roll):
    n = G * 8
    mid = g[n:, :LANES] + roll(g[n:, LANES:], 4, 0)
    tiles = [v.reshape(G, 8, LANES) for v in (g[:n, :LANES], mid, g[:n, LANES:])]
    return jnp.concatenate(tiles, axis=1).reshape(G * 24, LANES).astype(BF)


def unpack(x, roll):
    n = G * 8
    x = x.astype(F32).reshape(G, 24, LANES)
    first, mid, last = (x[:, 8 * j : 8 * j + 8].reshape(n, LANES) for j in range(3))
    return (
        jnp.concatenate((first, mid), axis=0).astype(BF),
        jnp.concatenate((last, roll(mid, n - 4, 0)), axis=0).astype(BF),
    )


def fold(x):
    x = x.reshape(G, YL, LINE)
    low, high = x[:, :4], x[:, 4:]
    parts = (low[:, :, :LANES], high[:, :, :LANES], low[:, :, LANES:], high[:, :, LANES:])
    return jnp.concatenate(parts, axis=2).astype(BF)


def unfold(x):
    x = x.astype(F32)
    half = LANES // 2
    low = jnp.concatenate((x[:, :, :LANES], x[:, :, 2 * LANES : 2 * LANES + half]), axis=2)
    high = jnp.concatenate((x[:, :, LANES : 2 * LANES], x[:, :, 2 * LANES + half :]), axis=2)
    return jnp.concatenate((low, high), axis=1).reshape(NY, LINE).astype(BF)


def stage1(p, s, table, roll):
    zero = jnp.zeros((LANES - ZL * YL, NX), BF)
    both = jnp.concatenate((p, zero, s, zero), axis=0)
    return pack(dot(table, both, 1, 1), roll)


def stage2(x, outer, inner, cw, sw, roll):
    n = LINE
    g = dot(outer, jnp.concatenate(unpack(x, roll), axis=1))
    parts = []
    for f in range(2):
        re, im = (g[j * n : (j + 1) * n, f * LANES : (f + 1) * LANES] for j in range(2))
        h = jnp.concatenate((re * cw + im * sw, im * cw - re * sw), axis=1).astype(BF)
        parts.append(dot(inner, h, 1, 1))
    return fold(jnp.concatenate(parts, axis=0))


def stage3(x, forward_y, back_y, wall, row_at, col_at):
    c = dot(forward_y, unfold(x))
    total = jnp.broadcast_to(wall, (LINE, NY)).T + wave_numbers(row_at, col_at)
    hat = c / jnp.where(row_at < G // 2, -total, 1.0 + DIFFUSION * total)
    return fold(dot(back_y, hat.astype(BF)))


def stage4(x, outer, inner, cw, sw, roll):
    z = unfold(x)
    parts = []
    for f in range(2):
        v = z[f * LANES : (f + 1) * LANES]
        h = dot(v, inner, 0, 0)
        re, im = h[:, :LANES], h[:, LANES:]
        parts.append(jnp.concatenate((re * cw - im * sw, im * cw + re * sw), axis=0).astype(BF))
    return pack(dot(outer, jnp.concatenate(parts, axis=1)), roll)


def stage5(x, table, roll):
    return tuple(dot(v, table, 0, 0)[: ZL * YL].astype(BF) for v in unpack(x, roll))


def turn(x, blocks):
    n = x.shape[0] // G * blocks
    return jnp.concatenate((x[n:], x[:n]), axis=0)


def call(fn, out, *args, axes=(None, None)):
    outs = out if isinstance(out, list) else [out]
    single = outs is not out

    def kernel(*refs):
        values = [r[...] for r in refs[: len(args)]]
        if axes[0]:
            values[0] = turn(values[0], G - FIRST[axes[0]])
        result = fn(*values)
        if axes[1]:
            result = turn(result, FIRST[axes[1]])
        for ref, value in zip(refs[len(args) :], (result,) if single else result, strict=True):
            ref[...] = value

    vmem = pl.BlockSpec(memory_space=pltpu.VMEM)
    make = pltpu.VMEM if axes[1] else jax.ShapeDtypeStruct
    shapes = tuple(make(s, BF) for s in outs)
    if axes[0]:
        args = [pltpu.with_memory_space_constraint(a, pltpu.VMEM) for a in args]
    result = pl.pallas_call(
        kernel,
        out_shape=shapes,
        in_specs=[vmem] * len(args),
        out_specs=(vmem,) * len(outs),
        name=fn.__name__,
    )(*args)
    return result[0] if single else result


def wave_numbers(row_at, col_at):
    item = lax.broadcasted_iota(jnp.int32, (1, LINE), 1)
    t = row_at % WAVES
    m = col_at * PER + item % PER
    n = item // PER + G * t
    signed = jnp.where(t < WAVES // 2, n, n - KEEP)
    kx_sq = (m.astype(F32) * (2.0 * math.pi / NX)) ** 2
    kz_sq = (signed.astype(F32) * (2.0 * math.pi / NZ)) ** 2
    return kz_sq + kx_sq


def shards(pressure_rhs, scalar_source, forward_y, back_y, wall_rates):
    fwd_x, back_x = (jnp.asarray(t, BF) for t in x_tables())
    outer_f, outer_b = jnp.asarray(z_outer(-1), BF), jnp.asarray(z_outer_back(), BF)
    inner_f, inner_b = jnp.asarray(z_inner(-1), BF), jnp.asarray(z_inner(1), BF)
    cw, sw = (jnp.asarray(t, F32) for t in twiddles())
    roll = pltpu.roll

    def exchange(x, axis):
        shape = x.shape
        x = x.reshape(G, -1, shape[-1])
        group = [(i + FIRST[axis]) % G for i in range(G)]
        x = lax.all_to_all(x, axis, split_axis=0, concat_axis=0, tiled=True, axis_index_groups=[group])
        return x.reshape(shape)

    def s1(*a):
        return stage1(*a, roll)

    def s2(*a):
        return stage2(*a, roll)

    def s3(*a):
        return stage3(*a, lax.axis_index("row"), lax.axis_index("col"))

    def s4(*a):
        return stage4(*a, roll)

    def s5(*a):
        return stage5(*a, roll)

    flat = (ZL * YL, NX)
    x = call(s1, (G * 24, LANES), pressure_rhs.reshape(flat), scalar_source.reshape(flat), fwd_x, axes=(None, "col"))
    x = exchange(x, "col")
    x = call(s2, (G, 4, 3 * LANES), x, outer_f, inner_f, cw, sw, axes=("col", "row"))
    x = exchange(x, "row")
    x = call(s3, (G, 4, 3 * LANES), x, forward_y, back_y, wall_rates.reshape(1, NY), axes=("row", "row"))
    x = exchange(x, "row")
    x = call(s4, (G * 24, LANES), x, outer_b, inner_b, cw, sw, axes=("row", "col"))
    x = exchange(x, "col")
    outs = call(s5, [flat, flat], x, back_x, axes=("col", None))
    return tuple(o.reshape(ZL, YL, NX) for o in outs)


def solution(mesh):
    field = P("col", "row", None)
    return jax.shard_map(
        shards,
        mesh=mesh,
        in_specs=(field, field, P(), P(), P()),
        out_specs=(field, field),
        check_vma=False,
    )
```

```python
import math

import jax
import jax.numpy as jnp
import numpy as np
from jax import lax
from jax.experimental import pallas as pl
from jax.experimental.pallas import tpu as pltpu
from jax.sharding import PartitionSpec as P

NX = 384
NY = 256
NZ = 384
KEEP = 256
DIFFUSION = 0.5
G = 32
ZL = NZ // G
YL = NY // G
PER = NX // 2 // G
ITEMS = 2 * PER
WAVES = KEEP // G
LINE = G * PER
LANES = 128
ORDER = {"row": [(23 + i) % G for i in range(G)], "col": [(20 + i) % G for i in range(G)]}
BF = jnp.bfloat16
F32 = jnp.float32

KEPT = np.array([t for t in range(NZ // G) if G * t < KEEP // 2 or G * t >= NZ - KEEP // 2])


def pairs(part_out, part_in, cos, sin, sign):
    if part_out == part_in:
        return cos
    return sign * sin if part_out == 1 else -sign * sin


def items():
    for i in range(ITEMS):
        yield i // 8, i % 8, i // PER, i % PER


def x_tables():
    fwd = np.zeros((2, G, 8, NX))
    back = np.zeros((2, G, 8, NX))
    x = np.arange(NX)
    factor = math.sqrt(2.0 / NX)
    for h, i, p, k in items():
        m = np.arange(G)[:, None] * PER + k
        angle = 2.0 * math.pi * (m * x[None, :] % NX) / NX
        value = factor * (np.cos(angle) if p == 0 else -np.sin(angle))
        fwd[h, :, i] = value
        back[h, :, i] = np.where(m == 0, 0.5, 1.0) * value
    return fwd.reshape(-1, NX), back.reshape(-1, NX)


def z_outer(sign):
    out = np.zeros((2, G, PER, 2, G, 8))
    angle = 2.0 * math.pi * (np.outer(np.arange(G), np.arange(G)) % G) / G
    cos, sin = np.cos(angle) / math.sqrt(G), np.sin(angle) / math.sqrt(G)
    for h, i, p, k in items():
        for q in range(2):
            out[q, :, k, h, :, i] = pairs(q, p, cos, sin, sign)
    return out.reshape(2 * LINE, 2 * G * 8)


def z_outer_back():
    out = np.zeros((2, G, 8, 2, G, PER))
    angle = 2.0 * math.pi * (np.outer(np.arange(G), np.arange(G)) % G) / G
    cos, sin = np.cos(angle) / math.sqrt(G), np.sin(angle) / math.sqrt(G)
    for h, i, p, k in items():
        for q in range(2):
            out[h, :, i, q, :, k] = pairs(p, q, cos, sin, 1)
    return out.reshape(2 * G * 8, 2 * LINE)


def z_inner(sign):
    out = np.zeros((2, WAVES, YL, 2, LANES))
    angle = 2.0 * math.pi * (np.outer(KEPT, np.arange(ZL)) % ZL) / ZL
    cos, sin = np.cos(angle) / math.sqrt(ZL), np.sin(angle) / math.sqrt(ZL)
    for a in range(2):
        for b in range(2):
            w = pairs(a, b, cos, sin, -1) if sign < 0 else pairs(b, a, cos, sin, 1)
            for y in range(YL):
                out[a, :, y, b, y : ZL * YL : YL] = w
    return out.reshape(2 * WAVES * YL, 2 * LANES)


def twiddles():
    angle = 2.0 * math.pi * np.outer(np.arange(G), np.arange(ZL)) / NZ
    angle = np.repeat(np.repeat(angle, PER, axis=0), YL, axis=1)
    angle = np.pad(angle, ((0, 0), (0, LANES - ZL * YL)))
    return np.cos(angle), np.sin(angle)


def dot(a, b, ca=1, cb=0):
    return lax.dot_general(a, b, (((ca,), (cb,)), ((), ())), preferred_element_type=F32)


def send(x, axis):
    return jnp.concatenate([x[i : i + 1] for i in ORDER[axis]], axis=0)


def receive(x, axis):
    place = [ORDER[axis].index(i) for i in range(G)]
    return jnp.concatenate([x[i : i + 1] for i in place], axis=0)


def pack(g, roll):
    n = G * 8
    mid = g[n:, :LANES] + roll(g[n:, LANES:], 4, 0)
    lane = lax.broadcasted_iota(jnp.int32, (n, LANES), 1)
    one, two = (roll(g[:n, LANES:], shift, 1) for shift in (96, 64))
    first = jnp.where(lane < 96, g[:n, :LANES], one).reshape(G, 2, 4, LANES)
    mid = jnp.where(lane < 96, mid, two).reshape(G, 2, 4, LANES)
    lane = lax.broadcasted_iota(jnp.int32, (G, 4, LANES), 2)
    low, high = two.reshape(G, 8, LANES)[:, :4], one.reshape(G, 8, LANES)[:, 4:]
    rest = jnp.where(lane < 32, low, high).reshape(G, 1, 4, LANES)
    return send(jnp.concatenate((first, mid, rest), axis=1), "col").astype(BF)


def unpack(x, roll):
    n = G * 8
    x = receive(x.astype(F32), "col")
    first, mid = x[:, :2].reshape(n, LANES), x[:, 2:4].reshape(n, LANES)
    rest = jnp.concatenate((x[:, 4], roll(x[:, 4], 96, 2)), axis=1).reshape(n, LANES)
    lane = lax.broadcasted_iota(jnp.int32, (n, LANES), 1)
    last = roll(jnp.where(lane < 32, rest, mid), 64, 1)
    last = jnp.where(lane < 32, roll(first, 32, 1), last)
    return (
        jnp.concatenate((first, mid), axis=0).astype(BF),
        jnp.concatenate((last, roll(mid, n - 4, 0)), axis=0).astype(BF),
    )


def fold(x):
    x = x.reshape(G, YL, LINE)
    low, high = x[:, :4], x[:, 4:]
    parts = (low[:, :, :LANES], high[:, :, :LANES], low[:, :, LANES:], high[:, :, LANES:])
    return send(jnp.concatenate(parts, axis=2), "row").astype(BF)


def unfold(x):
    x = receive(x.astype(F32), "row")
    half = LANES // 2
    low = jnp.concatenate((x[:, :, :LANES], x[:, :, 2 * LANES : 2 * LANES + half]), axis=2)
    high = jnp.concatenate((x[:, :, LANES : 2 * LANES], x[:, :, 2 * LANES + half :]), axis=2)
    return jnp.concatenate((low, high), axis=1).reshape(NY, LINE).astype(BF)


def stage1(p, s, table, roll):
    zero = jnp.zeros((LANES - ZL * YL, NX), BF)
    both = jnp.concatenate((p, zero, s, zero), axis=0)
    return pack(dot(table, both, 1, 1), roll)


def stage2(x, outer, inner, cw, sw, roll):
    n = LINE
    g = dot(outer, jnp.concatenate(unpack(x, roll), axis=1))
    parts = []
    for f in range(2):
        re, im = (g[j * n : (j + 1) * n, f * LANES : (f + 1) * LANES] for j in range(2))
        h = jnp.concatenate((re * cw + im * sw, im * cw - re * sw), axis=1).astype(BF)
        parts.append(dot(inner, h, 1, 1))
    return fold(jnp.concatenate(parts, axis=0))


def stage3(x, forward_y, back_y, wall, row_at, col_at):
    c = dot(forward_y, unfold(x))
    total = jnp.broadcast_to(wall, (LINE, NY)).T + wave_numbers(row_at, col_at)
    hat = c / jnp.where(row_at < G // 2, -total, 1.0 + DIFFUSION * total)
    return fold(dot(back_y, hat.astype(BF)))


def stage4(x, outer, inner, cw, sw, roll):
    z = unfold(x)
    parts = []
    for f in range(2):
        v = z[f * LANES : (f + 1) * LANES]
        h = dot(v, inner, 0, 0)
        re, im = h[:, :LANES], h[:, LANES:]
        parts.append(jnp.concatenate((re * cw - im * sw, im * cw + re * sw), axis=0).astype(BF))
    return pack(dot(outer, jnp.concatenate(parts, axis=1)), roll)


def stage5(x, table, roll):
    return tuple(dot(v, table, 0, 0)[: ZL * YL].astype(BF) for v in unpack(x, roll))


def call(fn, out, *args, fast=(True, True)):
    outs = out if isinstance(out, list) else [out]
    single = outs is not out

    def kernel(*refs):
        result = fn(*(r[...] for r in refs[: len(args)]))
        for ref, value in zip(refs[len(args) :], (result,) if single else result, strict=True):
            ref[...] = value

    vmem = pl.BlockSpec(memory_space=pltpu.VMEM)
    make = pltpu.VMEM if fast[1] else jax.ShapeDtypeStruct
    shapes = tuple(make(s, BF) for s in outs)
    if fast[0]:
        args = [pltpu.with_memory_space_constraint(a, pltpu.VMEM) for a in args]
    result = pl.pallas_call(
        kernel,
        out_shape=shapes,
        in_specs=[vmem] * len(args),
        out_specs=(vmem,) * len(outs),
        name=fn.__name__,
    )(*args)
    return result[0] if single else result


def wave_numbers(row_at, col_at):
    item = lax.broadcasted_iota(jnp.int32, (1, LINE), 1)
    t = row_at % WAVES
    m = col_at * PER + item % PER
    n = item // PER + G * t
    signed = jnp.where(t < WAVES // 2, n, n - KEEP)
    kx_sq = (m.astype(F32) * (2.0 * math.pi / NX)) ** 2
    kz_sq = (signed.astype(F32) * (2.0 * math.pi / NZ)) ** 2
    return kz_sq + kx_sq


def shards(pressure_rhs, scalar_source, forward_y, back_y, wall_rates):
    fwd_x, back_x = (jnp.asarray(t, BF) for t in x_tables())
    outer_f, outer_b = jnp.asarray(z_outer(-1), BF), jnp.asarray(z_outer_back(), BF)
    inner_f, inner_b = jnp.asarray(z_inner(-1), BF), jnp.asarray(z_inner(1), BF)
    cw, sw = (jnp.asarray(t, F32) for t in twiddles())
    roll = pltpu.roll

    def exchange(x, axis):
        return lax.all_to_all(x, axis, split_axis=0, concat_axis=0, tiled=True, axis_index_groups=[ORDER[axis]])

    def s1(*a):
        return stage1(*a, roll)

    def s2(*a):
        return stage2(*a, roll)

    def s3(*a):
        return stage3(*a, lax.axis_index("row"), lax.axis_index("col"))

    def s4(*a):
        return stage4(*a, roll)

    def s5(*a):
        return stage5(*a, roll)

    flat = (ZL * YL, NX)
    x = call(s1, (G, 5, 4, LANES), pressure_rhs.reshape(flat), scalar_source.reshape(flat), fwd_x, fast=(False, True))
    x = exchange(x, "col")
    x = call(s2, (G, 4, 3 * LANES), x, outer_f, inner_f, cw, sw)
    x = exchange(x, "row")
    x = call(s3, (G, 4, 3 * LANES), x, forward_y, back_y, wall_rates.reshape(1, NY))
    x = exchange(x, "row")
    x = call(s4, (G, 5, 4, LANES), x, outer_b, inner_b, cw, sw)
    x = exchange(x, "col")
    outs = call(s5, [flat, flat], x, back_x, fast=(True, False))
    return tuple(o.reshape(ZL, YL, NX) for o in outs)


def solution(mesh):
    field = P("col", "row", None)
    return jax.shard_map(
        shards,
        mesh=mesh,
        in_specs=(field, field, P(), P(), P()),
        out_specs=(field, field),
        check_vma=False,
    )
```

```python
import math

import jax
import jax.numpy as jnp
import numpy as np
from jax import lax
from jax.experimental import pallas as pl
from jax.experimental.pallas import tpu as pltpu
from jax.sharding import PartitionSpec as P

NX = 384
NY = 256
NZ = 384
KEEP = 256
DIFFUSION = 0.5
G = 32
ZL = NZ // G
YL = NY // G
PER = NX // 2 // G
ITEMS = 2 * PER
WAVES = KEEP // G
LINE = G * PER
LANES = 128
ORDER = {"row": [(21 + i) % G for i in range(G)], "col": [(20 + i) % G for i in range(G)]}
BF = jnp.bfloat16
F32 = jnp.float32

KEPT = np.array([t for t in range(NZ // G) if G * t < KEEP // 2 or G * t >= NZ - KEEP // 2])


def pairs(part_out, part_in, cos, sin, sign):
    if part_out == part_in:
        return cos
    return sign * sin if part_out == 1 else -sign * sin


def items():
    for i in range(ITEMS):
        yield i // 8, i % 8, i // PER, i % PER


def x_tables():
    fwd = np.zeros((2, G, 8, NX))
    back = np.zeros((2, G, 8, NX))
    x = np.arange(NX)
    factor = math.sqrt(2.0 / NX)
    for h, i, p, k in items():
        m = np.arange(G)[:, None] * PER + k
        angle = 2.0 * math.pi * (m * x[None, :] % NX) / NX
        value = factor * (np.cos(angle) if p == 0 else -np.sin(angle))
        fwd[h, :, i] = value
        back[h, :, i] = np.where(m == 0, 0.5, 1.0) * value
    return fwd.reshape(-1, NX), back.reshape(-1, NX)


def z_outer(sign):
    out = np.zeros((2, G, PER, 2, G, 8))
    angle = 2.0 * math.pi * (np.outer(np.arange(G), np.arange(G)) % G) / G
    cos, sin = np.cos(angle) / math.sqrt(G), np.sin(angle) / math.sqrt(G)
    for h, i, p, k in items():
        for q in range(2):
            out[q, :, k, h, :, i] = pairs(q, p, cos, sin, sign)
    return out.reshape(2 * LINE, 2 * G * 8)


def z_outer_back():
    out = np.zeros((2, G, 8, 2, G, PER))
    angle = 2.0 * math.pi * (np.outer(np.arange(G), np.arange(G)) % G) / G
    cos, sin = np.cos(angle) / math.sqrt(G), np.sin(angle) / math.sqrt(G)
    for h, i, p, k in items():
        for q in range(2):
            out[h, :, i, q, :, k] = pairs(p, q, cos, sin, 1)
    return out.reshape(2 * G * 8, 2 * LINE)


def z_inner(sign):
    out = np.zeros((2, WAVES, YL, 2, LANES))
    angle = 2.0 * math.pi * (np.outer(KEPT, np.arange(ZL)) % ZL) / ZL
    cos, sin = np.cos(angle) / math.sqrt(ZL), np.sin(angle) / math.sqrt(ZL)
    for a in range(2):
        for b in range(2):
            w = pairs(a, b, cos, sin, -1) if sign < 0 else pairs(b, a, cos, sin, 1)
            for y in range(YL):
                out[a, :, y, b, y : ZL * YL : YL] = w
    return out.reshape(2 * WAVES * YL, 2 * LANES)


def twiddles():
    angle = 2.0 * math.pi * np.outer(np.arange(G), np.arange(ZL)) / NZ
    angle = np.repeat(np.repeat(angle, PER, axis=0), YL, axis=1)
    angle = np.pad(angle, ((0, 0), (0, LANES - ZL * YL)))
    return np.cos(angle), np.sin(angle)


def dot(a, b, ca=1, cb=0):
    return lax.dot_general(a, b, (((ca,), (cb,)), ((), ())), preferred_element_type=F32)


def send(x, axis):
    return jnp.concatenate([x[i : i + 1] for i in ORDER[axis]], axis=0)


def receive(x, axis):
    place = [ORDER[axis].index(i) for i in range(G)]
    return jnp.concatenate([x[i : i + 1] for i in place], axis=0)


def pack(g, roll):
    n = G * 8
    mid = g[n:, :LANES] + roll(g[n:, LANES:], 4, 0)
    lane = lax.broadcasted_iota(jnp.int32, (n, LANES), 1)
    one, two = (roll(g[:n, LANES:], shift, 1) for shift in (96, 64))
    first = jnp.where(lane < 96, g[:n, :LANES], one).reshape(G, 2, 4, LANES)
    mid = jnp.where(lane < 96, mid, two).reshape(G, 2, 4, LANES)
    lane = lax.broadcasted_iota(jnp.int32, (G, 4, LANES), 2)
    low, high = two.reshape(G, 8, LANES)[:, :4], one.reshape(G, 8, LANES)[:, 4:]
    rest = jnp.where(lane < 32, low, high).reshape(G, 1, 4, LANES)
    return send(jnp.concatenate((first, mid, rest), axis=1), "col").astype(BF)


def unpack(x, roll):
    n = G * 8
    x = receive(x.astype(F32), "col")
    first, mid = x[:, :2].reshape(n, LANES), x[:, 2:4].reshape(n, LANES)
    rest = jnp.concatenate((x[:, 4], roll(x[:, 4], 96, 2)), axis=1).reshape(n, LANES)
    lane = lax.broadcasted_iota(jnp.int32, (n, LANES), 1)
    last = roll(jnp.where(lane < 32, rest, mid), 64, 1)
    last = jnp.where(lane < 32, roll(first, 32, 1), last)
    return (
        jnp.concatenate((first, mid), axis=0).astype(BF),
        jnp.concatenate((last, roll(mid, n - 4, 0)), axis=0).astype(BF),
    )


def fold(x):
    x = x.reshape(G, YL, LINE)
    low, high = x[:, :4], x[:, 4:]
    parts = (low[:, :, :LANES], high[:, :, :LANES], low[:, :, LANES:], high[:, :, LANES:])
    return send(jnp.concatenate(parts, axis=2), "row").astype(BF)


def unfold(x):
    x = receive(x.astype(F32), "row")
    half = LANES // 2
    low = jnp.concatenate((x[:, :, :LANES], x[:, :, 2 * LANES : 2 * LANES + half]), axis=2)
    high = jnp.concatenate((x[:, :, LANES : 2 * LANES], x[:, :, 2 * LANES + half :]), axis=2)
    return jnp.concatenate((low, high), axis=1).reshape(NY, LINE).astype(BF)


def stage1(p, s, table, roll):
    zero = jnp.zeros((LANES - ZL * YL, NX), BF)
    both = jnp.concatenate((p, zero, s, zero), axis=0)
    return pack(dot(table, both, 1, 1), roll)


def stage2(x, outer, inner, cw, sw, roll):
    n = LINE
    g = dot(outer, jnp.concatenate(unpack(x, roll), axis=1))
    parts = []
    for f in range(2):
        re, im = (g[j * n : (j + 1) * n, f * LANES : (f + 1) * LANES] for j in range(2))
        h = jnp.concatenate((re * cw + im * sw, im * cw - re * sw), axis=1).astype(BF)
        parts.append(dot(inner, h, 1, 1))
    return fold(jnp.concatenate(parts, axis=0))


def stage3(x, forward_y, back_y, wall, row_at, col_at):
    c = dot(forward_y, unfold(x))
    total = jnp.broadcast_to(wall, (LINE, NY)).T + wave_numbers(row_at, col_at)
    hat = c / jnp.where(row_at < G // 2, -total, 1.0 + DIFFUSION * total)
    return fold(dot(back_y, hat.astype(BF)))


def stage4(x, outer, inner, cw, sw, roll):
    z = unfold(x)
    parts = []
    for f in range(2):
        v = z[f * LANES : (f + 1) * LANES]
        h = dot(v, inner, 0, 0)
        re, im = h[:, :LANES], h[:, LANES:]
        parts.append(jnp.concatenate((re * cw - im * sw, im * cw + re * sw), axis=0).astype(BF))
    return pack(dot(outer, jnp.concatenate(parts, axis=1)), roll)


def stage5(x, table, roll):
    return tuple(dot(v, table, 0, 0)[: ZL * YL].astype(BF) for v in unpack(x, roll))


def call(fn, out, *args, fast=(True, True)):
    outs = out if isinstance(out, list) else [out]
    single = outs is not out

    def kernel(*refs):
        result = fn(*(r[...] for r in refs[: len(args)]))
        for ref, value in zip(refs[len(args) :], (result,) if single else result, strict=True):
            ref[...] = value

    vmem = pl.BlockSpec(memory_space=pltpu.VMEM)
    make = pltpu.VMEM if fast[1] else jax.ShapeDtypeStruct
    shapes = tuple(make(s, BF) for s in outs)
    if fast[0]:
        args = [pltpu.with_memory_space_constraint(a, pltpu.VMEM) for a in args]
    result = pl.pallas_call(
        kernel,
        out_shape=shapes,
        in_specs=[vmem] * len(args),
        out_specs=(vmem,) * len(outs),
        name=fn.__name__,
    )(*args)
    return result[0] if single else result


def wave_numbers(row_at, col_at):
    item = lax.broadcasted_iota(jnp.int32, (1, LINE), 1)
    t = row_at % WAVES
    m = col_at * PER + item % PER
    n = item // PER + G * t
    signed = jnp.where(t < WAVES // 2, n, n - KEEP)
    kx_sq = (m.astype(F32) * (2.0 * math.pi / NX)) ** 2
    kz_sq = (signed.astype(F32) * (2.0 * math.pi / NZ)) ** 2
    return kz_sq + kx_sq


def shards(pressure_rhs, scalar_source, forward_y, back_y, wall_rates):
    fwd_x, back_x = (jnp.asarray(t, BF) for t in x_tables())
    outer_f, outer_b = jnp.asarray(z_outer(-1), BF), jnp.asarray(z_outer_back(), BF)
    inner_f, inner_b = jnp.asarray(z_inner(-1), BF), jnp.asarray(z_inner(1), BF)
    cw, sw = (jnp.asarray(t, F32) for t in twiddles())
    roll = pltpu.roll

    def exchange(x, axis):
        return lax.all_to_all(x, axis, split_axis=0, concat_axis=0, tiled=True, axis_index_groups=[ORDER[axis]])

    def s1(*a):
        return stage1(*a, roll)

    def s2(*a):
        return stage2(*a, roll)

    def s3(*a):
        return stage3(*a, lax.axis_index("row"), lax.axis_index("col"))

    def s4(*a):
        return stage4(*a, roll)

    def s5(*a):
        return stage5(*a, roll)

    flat = (ZL * YL, NX)
    x = call(s1, (G, 5, 4, LANES), pressure_rhs.reshape(flat), scalar_source.reshape(flat), fwd_x, fast=(False, True))
    x = exchange(x, "col")
    x = call(s2, (G, 4, 3 * LANES), x, outer_f, inner_f, cw, sw)
    x = exchange(x, "row")
    x = call(s3, (G, 4, 3 * LANES), x, forward_y, back_y, wall_rates.reshape(1, NY))
    x = exchange(x, "row")
    x = call(s4, (G, 5, 4, LANES), x, outer_b, inner_b, cw, sw)
    x = exchange(x, "col")
    outs = call(s5, [flat, flat], x, back_x, fast=(True, False))
    return tuple(o.reshape(ZL, YL, NX) for o in outs)


def solution(mesh):
    field = P("col", "row", None)
    return jax.shard_map(
        shards,
        mesh=mesh,
        in_specs=(field, field, P(), P(), P()),
        out_specs=(field, field),
        check_vma=False,
    )
```

```python
import math

import jax
import jax.numpy as jnp
import numpy as np
from jax import lax
from jax.experimental import pallas as pl
from jax.experimental.pallas import tpu as pltpu
from jax.sharding import PartitionSpec as P

NX = 384
NY = 256
NZ = 384
KEEP = 256
DIFFUSION = 0.5
G = 32
ZL = NZ // G
YL = NY // G
PER = NX // 2 // G
ITEMS = 2 * PER
WAVES = KEEP // G
LINE = G * PER
LANES = 128
ORDER = {"row": [(21 + i) % G for i in range(G)], "col": [(20 + i) % G for i in range(G)]}
BF = jnp.bfloat16
F32 = jnp.float32

KEPT = np.array([t for t in range(NZ // G) if G * t < KEEP // 2 or G * t >= NZ - KEEP // 2])


def pairs(part_out, part_in, cos, sin, sign):
    if part_out == part_in:
        return cos
    return sign * sin if part_out == 1 else -sign * sin


def items():
    for i in range(ITEMS):
        yield i // 8, i % 8, i // PER, i % PER


def x_tables():
    fwd = np.zeros((2, G, 8, NX))
    back = np.zeros((2, G, 8, NX))
    x = np.arange(NX)
    factor = math.sqrt(2.0 / NX)
    for h, i, p, k in items():
        m = np.arange(G)[:, None] * PER + k
        angle = 2.0 * math.pi * (m * x[None, :] % NX) / NX
        value = factor * (np.cos(angle) if p == 0 else -np.sin(angle))
        fwd[h, :, i] = value
        back[h, :, i] = np.where(m == 0, 0.5, 1.0) * value
    return fwd.reshape(-1, NX), back.reshape(-1, NX)


def z_outer(sign):
    out = np.zeros((2, G, PER, 2, G, 8))
    angle = 2.0 * math.pi * (np.outer(np.arange(G), np.arange(G)) % G) / G
    cos, sin = np.cos(angle) / math.sqrt(G), np.sin(angle) / math.sqrt(G)
    for h, i, p, k in items():
        for q in range(2):
            out[q, :, k, h, :, i] = pairs(q, p, cos, sin, sign)
    return out.reshape(2 * LINE, 2 * G * 8)


def z_outer_back():
    out = np.zeros((2, G, 8, 2, G, PER))
    angle = 2.0 * math.pi * (np.outer(np.arange(G), np.arange(G)) % G) / G
    cos, sin = np.cos(angle) / math.sqrt(G), np.sin(angle) / math.sqrt(G)
    for h, i, p, k in items():
        for q in range(2):
            out[h, :, i, q, :, k] = pairs(p, q, cos, sin, 1)
    return out.reshape(2 * G * 8, 2 * LINE)


def z_inner(sign):
    out = np.zeros((2, WAVES, YL, 2, LANES))
    angle = 2.0 * math.pi * (np.outer(KEPT, np.arange(ZL)) % ZL) / ZL
    cos, sin = np.cos(angle) / math.sqrt(ZL), np.sin(angle) / math.sqrt(ZL)
    for a in range(2):
        for b in range(2):
            w = pairs(a, b, cos, sin, -1) if sign < 0 else pairs(b, a, cos, sin, 1)
            for y in range(YL):
                out[a, :, y, b, y : ZL * YL : YL] = w
    return out.reshape(2 * WAVES * YL, 2 * LANES)


def twiddles():
    angle = 2.0 * math.pi * np.outer(np.arange(G), np.arange(ZL)) / NZ
    angle = np.repeat(np.repeat(angle, PER, axis=0), YL, axis=1)
    angle = np.pad(angle, ((0, 0), (0, LANES - ZL * YL)))
    return np.cos(angle), np.sin(angle)


def dot(a, b, ca=1, cb=0):
    return lax.dot_general(a, b, (((ca,), (cb,)), ((), ())), preferred_element_type=F32)


def send(x, axis):
    return jnp.concatenate([x[i : i + 1] for i in ORDER[axis]], axis=0)


def receive(x, axis):
    place = [ORDER[axis].index(i) for i in range(G)]
    return jnp.concatenate([x[i : i + 1] for i in place], axis=0)


def pack(g, roll):
    n = G * 8
    mid = g[n:, :LANES] + roll(g[n:, LANES:], 4, 0)
    lane = lax.broadcasted_iota(jnp.int32, (n, LANES), 1)
    one, two = (roll(g[:n, LANES:], shift, 1) for shift in (96, 64))
    first = jnp.where(lane < 96, g[:n, :LANES], one).reshape(G, 2, 4, LANES)
    mid = jnp.where(lane < 96, mid, two).reshape(G, 2, 4, LANES)
    lane = lax.broadcasted_iota(jnp.int32, (G, 4, LANES), 2)
    low, high = g[:n, LANES:].reshape(G, 8, LANES)[:, :4], two.reshape(G, 8, LANES)[:, 4:]
    rest = jnp.where(lane < 64, high, low).reshape(G, 1, 4, LANES)
    return send(jnp.concatenate((first, mid, rest), axis=1), "col").astype(BF)


def unpack(x, roll):
    n = G * 8
    x = receive(x.astype(F32), "col")
    first, mid = x[:, :2].reshape(n, LANES), x[:, 2:4].reshape(n, LANES)
    rest = jnp.concatenate((x[:, 4], x[:, 4]), axis=1).reshape(n, LANES)
    lane = lax.broadcasted_iota(jnp.int32, (n, LANES), 1)
    low = lax.broadcasted_iota(jnp.int32, (n, LANES), 0) % 8 < 4
    last = roll(jnp.where(lane < 32, rest, mid), 64, 1)
    last = jnp.where(lane < 32, roll(first, 32, 1), jnp.where((lane >= 64) & low, rest, last))
    return (
        jnp.concatenate((first, mid), axis=0).astype(BF),
        jnp.concatenate((last, roll(mid, n - 4, 0)), axis=0).astype(BF),
    )


def fold(x):
    x = x.reshape(G, YL, LINE)
    low, high = x[:, :4], x[:, 4:]
    parts = (low[:, :, :LANES], high[:, :, :LANES], low[:, :, LANES:], high[:, :, LANES:])
    return send(jnp.concatenate(parts, axis=2), "row").astype(BF)


def unfold(x):
    x = receive(x.astype(F32), "row")
    half = LANES // 2
    low = jnp.concatenate((x[:, :, :LANES], x[:, :, 2 * LANES : 2 * LANES + half]), axis=2)
    high = jnp.concatenate((x[:, :, LANES : 2 * LANES], x[:, :, 2 * LANES + half :]), axis=2)
    return jnp.concatenate((low, high), axis=1).reshape(NY, LINE).astype(BF)


def stage1(p, s, table, roll):
    zero = jnp.zeros((LANES - ZL * YL, NX), BF)
    both = jnp.concatenate((p, zero, s, zero), axis=0)
    return pack(dot(table, both, 1, 1), roll)


def stage2(x, outer, inner, cw, sw, roll):
    n = LINE
    g = dot(outer, jnp.concatenate(unpack(x, roll), axis=1))
    parts = []
    for f in range(2):
        re, im = (g[j * n : (j + 1) * n, f * LANES : (f + 1) * LANES] for j in range(2))
        h = jnp.concatenate((re * cw + im * sw, im * cw - re * sw), axis=1).astype(BF)
        parts.append(dot(inner, h, 1, 1))
    return fold(jnp.concatenate(parts, axis=0))


def stage3(x, forward_y, back_y, wall, row_at, col_at):
    c = dot(forward_y, unfold(x))
    total = jnp.broadcast_to(wall, (LINE, NY)).T + wave_numbers(row_at, col_at)
    hat = c / jnp.where(row_at < G // 2, -total, 1.0 + DIFFUSION * total)
    return fold(dot(back_y, hat.astype(BF)))


def stage4(x, outer, inner, cw, sw, roll):
    z = unfold(x)
    parts = []
    for f in range(2):
        v = z[f * LANES : (f + 1) * LANES]
        h = dot(v, inner, 0, 0)
        re, im = h[:, :LANES], h[:, LANES:]
        parts.append(jnp.concatenate((re * cw - im * sw, im * cw + re * sw), axis=0).astype(BF))
    return pack(dot(outer, jnp.concatenate(parts, axis=1)), roll)


def stage5(x, table, roll):
    return tuple(dot(v, table, 0, 0)[: ZL * YL].astype(BF) for v in unpack(x, roll))


def call(fn, out, *args, fast=(True, True)):
    outs = out if isinstance(out, list) else [out]
    single = outs is not out

    def kernel(*refs):
        result = fn(*(r[...] for r in refs[: len(args)]))
        for ref, value in zip(refs[len(args) :], (result,) if single else result, strict=True):
            ref[...] = value

    vmem = pl.BlockSpec(memory_space=pltpu.VMEM)
    make = pltpu.VMEM if fast[1] else jax.ShapeDtypeStruct
    shapes = tuple(make(s, BF) for s in outs)
    if fast[0]:
        args = [pltpu.with_memory_space_constraint(a, pltpu.VMEM) for a in args]
    result = pl.pallas_call(
        kernel,
        out_shape=shapes,
        in_specs=[vmem] * len(args),
        out_specs=(vmem,) * len(outs),
        name=fn.__name__,
    )(*args)
    return result[0] if single else result


def wave_numbers(row_at, col_at):
    item = lax.broadcasted_iota(jnp.int32, (1, LINE), 1)
    t = row_at % WAVES
    m = col_at * PER + item % PER
    n = item // PER + G * t
    signed = jnp.where(t < WAVES // 2, n, n - KEEP)
    kx_sq = (m.astype(F32) * (2.0 * math.pi / NX)) ** 2
    kz_sq = (signed.astype(F32) * (2.0 * math.pi / NZ)) ** 2
    return kz_sq + kx_sq


def shards(pressure_rhs, scalar_source, forward_y, back_y, wall_rates):
    fwd_x, back_x = (jnp.asarray(t, BF) for t in x_tables())
    outer_f, outer_b = jnp.asarray(z_outer(-1), BF), jnp.asarray(z_outer_back(), BF)
    inner_f, inner_b = jnp.asarray(z_inner(-1), BF), jnp.asarray(z_inner(1), BF)
    cw, sw = (jnp.asarray(t, F32) for t in twiddles())
    roll = pltpu.roll

    def exchange(x, axis):
        return lax.all_to_all(x, axis, split_axis=0, concat_axis=0, tiled=True, axis_index_groups=[ORDER[axis]])

    def s1(*a):
        return stage1(*a, roll)

    def s2(*a):
        return stage2(*a, roll)

    def s3(*a):
        return stage3(*a, lax.axis_index("row"), lax.axis_index("col"))

    def s4(*a):
        return stage4(*a, roll)

    def s5(*a):
        return stage5(*a, roll)

    flat = (ZL * YL, NX)
    x = call(s1, (G, 5, 4, LANES), pressure_rhs.reshape(flat), scalar_source.reshape(flat), fwd_x, fast=(False, True))
    x = exchange(x, "col")
    x = call(s2, (G, 4, 3 * LANES), x, outer_f, inner_f, cw, sw)
    x = exchange(x, "row")
    x = call(s3, (G, 4, 3 * LANES), x, forward_y, back_y, wall_rates.reshape(1, NY))
    x = exchange(x, "row")
    x = call(s4, (G, 5, 4, LANES), x, outer_b, inner_b, cw, sw)
    x = exchange(x, "col")
    outs = call(s5, [flat, flat], x, back_x, fast=(True, False))
    return tuple(o.reshape(ZL, YL, NX) for o in outs)


def solution(mesh):
    field = P("col", "row", None)
    return jax.shard_map(
        shards,
        mesh=mesh,
        in_specs=(field, field, P(), P(), P()),
        out_specs=(field, field),
        check_vma=False,
    )
```

```python
import math

import jax
import jax.numpy as jnp
import numpy as np
from jax import lax
from jax.experimental import pallas as pl
from jax.experimental.pallas import tpu as pltpu
from jax.sharding import PartitionSpec as P

NX = 384
NY = 256
NZ = 384
KEEP = 256
DIFFUSION = 0.5
G = 32
ZL = NZ // G
YL = NY // G
PER = NX // 2 // G
ITEMS = 2 * PER
WAVES = KEEP // G
LINE = G * PER
LANES = 128
ORDER = {"row": [(21 + i) % G for i in range(G)], "col": [(20 + i) % G for i in range(G)]}
BF = jnp.bfloat16
F32 = jnp.float32

KEPT = np.array([t for t in range(NZ // G) if G * t < KEEP // 2 or G * t >= NZ - KEEP // 2])


def pairs(part_out, part_in, cos, sin, sign):
    if part_out == part_in:
        return cos
    return sign * sin if part_out == 1 else -sign * sin


def items():
    for i in range(ITEMS):
        yield i // 8, i % 8, i // PER, i % PER


def x_tables():
    fwd = np.zeros((2, G, 8, NX))
    back = np.zeros((2, G, 8, NX))
    x = np.arange(NX)
    factor = math.sqrt(2.0 / NX)
    for h, i, p, k in items():
        m = np.arange(G)[:, None] * PER + k
        angle = 2.0 * math.pi * (m * x[None, :] % NX) / NX
        value = factor * (np.cos(angle) if p == 0 else -np.sin(angle))
        fwd[h, :, i] = value
        back[h, :, i] = np.where(m == 0, 0.5, 1.0) * value
    return fwd.reshape(-1, NX), back.reshape(-1, NX)


def z_outer(sign):
    out = np.zeros((2, G, PER, 2, G, 8))
    angle = 2.0 * math.pi * (np.outer(np.arange(G), np.arange(G)) % G) / G
    cos, sin = np.cos(angle) / math.sqrt(G), np.sin(angle) / math.sqrt(G)
    for h, i, p, k in items():
        for q in range(2):
            out[q, :, k, h, :, i] = pairs(q, p, cos, sin, sign)
    return out.reshape(2 * LINE, 2 * G * 8)


def z_outer_back():
    out = np.zeros((2, G, 8, 2, G, PER))
    angle = 2.0 * math.pi * (np.outer(np.arange(G), np.arange(G)) % G) / G
    cos, sin = np.cos(angle) / math.sqrt(G), np.sin(angle) / math.sqrt(G)
    for h, i, p, k in items():
        for q in range(2):
            out[h, :, i, q, :, k] = pairs(p, q, cos, sin, 1)
    return out.reshape(2 * G * 8, 2 * LINE)


def z_inner(sign):
    out = np.zeros((2, WAVES, YL, 2, LANES))
    angle = 2.0 * math.pi * (np.outer(KEPT, np.arange(ZL)) % ZL) / ZL
    cos, sin = np.cos(angle) / math.sqrt(ZL), np.sin(angle) / math.sqrt(ZL)
    for a in range(2):
        for b in range(2):
            w = pairs(a, b, cos, sin, -1) if sign < 0 else pairs(b, a, cos, sin, 1)
            for y in range(YL):
                out[a, :, y, b, y : ZL * YL : YL] = w
    return out.reshape(2 * WAVES * YL, 2 * LANES)


def twiddles():
    angle = 2.0 * math.pi * np.outer(np.arange(G), np.arange(ZL)) / NZ
    angle = np.repeat(np.repeat(angle, PER, axis=0), YL, axis=1)
    angle = np.pad(angle, ((0, 0), (0, LANES - ZL * YL)))
    return np.cos(angle), np.sin(angle)


def dot(a, b, ca=1, cb=0):
    return lax.dot_general(a, b, (((ca,), (cb,)), ((), ())), preferred_element_type=F32)


def send(x, axis):
    return jnp.concatenate([x[i : i + 1] for i in ORDER[axis]], axis=0)


def receive(x, axis):
    place = [ORDER[axis].index(i) for i in range(G)]
    return jnp.concatenate([x[i : i + 1] for i in place], axis=0)


def pack(g, roll):
    n = G * 8
    mid = g[n:, :LANES] + roll(g[n:, LANES:], 4, 0)
    lane = lax.broadcasted_iota(jnp.int32, (n, LANES), 1)
    one, two = (roll(g[:n, LANES:], shift, 1) for shift in (96, 64))
    first = jnp.where(lane < 96, g[:n, :LANES], one).reshape(G, 2, 4, LANES)
    mid = jnp.where(lane < 96, mid, two).reshape(G, 2, 4, LANES)
    lane = lax.broadcasted_iota(jnp.int32, (G, 4, LANES), 2)
    low, high = g[:n, LANES:].reshape(G, 8, LANES)[:, :4], two.reshape(G, 8, LANES)[:, 4:]
    rest = jnp.where(lane < 64, high, low).reshape(G, 1, 4, LANES)
    return send(jnp.concatenate((first, mid, rest), axis=1), "col").astype(BF)


def unpack(x, roll):
    n = G * 8
    x = receive(x.astype(F32), "col")
    first, mid = x[:, :2].reshape(n, LANES), x[:, 2:4].reshape(n, LANES)
    rest = jnp.concatenate((x[:, 4], x[:, 4]), axis=1).reshape(n, LANES)
    lane = lax.broadcasted_iota(jnp.int32, (n, LANES), 1)
    low = lax.broadcasted_iota(jnp.int32, (n, LANES), 0) % 8 < 4
    last = roll(jnp.where(lane < 32, rest, mid), 64, 1)
    last = jnp.where(lane < 32, roll(first, 32, 1), jnp.where((lane >= 64) & low, rest, last))
    return (
        jnp.concatenate((first, mid), axis=0).astype(BF),
        jnp.concatenate((last, roll(mid, n - 4, 0)), axis=0).astype(BF),
    )


def fold(x):
    x = x.reshape(G, YL, LINE)
    low, high = x[:, :4], x[:, 4:]
    parts = (low[:, :, :LANES], high[:, :, :LANES], low[:, :, LANES:], high[:, :, LANES:])
    return send(jnp.concatenate(parts, axis=2), "row").astype(BF)


def unfold(x):
    x = receive(x.astype(F32), "row")
    half = LANES // 2
    low = jnp.concatenate((x[:, :, :LANES], x[:, :, 2 * LANES : 2 * LANES + half]), axis=2)
    high = jnp.concatenate((x[:, :, LANES : 2 * LANES], x[:, :, 2 * LANES + half :]), axis=2)
    return jnp.concatenate((low, high), axis=1).reshape(NY, LINE).astype(BF)


def stage1(p, s, table, roll):
    zero = jnp.zeros((LANES - ZL * YL, NX), BF)
    both = jnp.concatenate((p, zero, s, zero), axis=0)
    return pack(dot(table, both, 1, 1), roll)


def stage2(x, outer, inner, cw, sw, roll):
    n = LINE
    g = dot(outer, jnp.concatenate(unpack(x, roll), axis=1))
    parts = []
    for f in range(2):
        re, im = (g[j * n : (j + 1) * n, f * LANES : (f + 1) * LANES] for j in range(2))
        h = jnp.concatenate((re * cw + im * sw, im * cw - re * sw), axis=1).astype(BF)
        parts.append(dot(inner, h, 1, 1))
    return fold(jnp.concatenate(parts, axis=0))


def stage3(x, forward_y, back_y, wall, row_at, col_at):
    c = dot(forward_y, unfold(x))
    wall = jnp.broadcast_to(wall, (LANES, NY)).T
    wall = jnp.concatenate((wall, wall[:, : LINE - LANES]), axis=1)
    total = wall + wave_numbers(row_at, col_at)
    hat = c / jnp.where(row_at < G // 2, -total, 1.0 + DIFFUSION * total)
    return fold(dot(back_y, hat.astype(BF)))


def stage4(x, outer, inner, cw, sw, roll):
    z = unfold(x)
    parts = []
    for f in range(2):
        v = z[f * LANES : (f + 1) * LANES]
        h = dot(v, inner, 0, 0)
        re, im = h[:, :LANES], h[:, LANES:]
        parts.append(jnp.concatenate((re * cw - im * sw, im * cw + re * sw), axis=0).astype(BF))
    return pack(dot(outer, jnp.concatenate(parts, axis=1)), roll)


def stage5(x, table, roll):
    return tuple(dot(v, table, 0, 0)[: ZL * YL].astype(BF) for v in unpack(x, roll))


def call(fn, out, *args, fast=(True, True)):
    outs = out if isinstance(out, list) else [out]
    single = outs is not out

    def kernel(*refs):
        result = fn(*(r[...] for r in refs[: len(args)]))
        for ref, value in zip(refs[len(args) :], (result,) if single else result, strict=True):
            ref[...] = value

    vmem = pl.BlockSpec(memory_space=pltpu.VMEM)
    make = pltpu.VMEM if fast[1] else jax.ShapeDtypeStruct
    shapes = tuple(make(s, BF) for s in outs)
    if fast[0]:
        args = [pltpu.with_memory_space_constraint(a, pltpu.VMEM) for a in args]
    result = pl.pallas_call(
        kernel,
        out_shape=shapes,
        in_specs=[vmem] * len(args),
        out_specs=(vmem,) * len(outs),
        name=fn.__name__,
    )(*args)
    return result[0] if single else result


def wave_numbers(row_at, col_at):
    item = lax.broadcasted_iota(jnp.int32, (1, LINE), 1)
    t = row_at % WAVES
    m = col_at * PER + item % PER
    n = item // PER + G * t
    signed = jnp.where(t < WAVES // 2, n, n - KEEP)
    kx_sq = (m.astype(F32) * (2.0 * math.pi / NX)) ** 2
    kz_sq = (signed.astype(F32) * (2.0 * math.pi / NZ)) ** 2
    return kz_sq + kx_sq


def shards(pressure_rhs, scalar_source, forward_y, back_y, wall_rates):
    fwd_x, back_x = (jnp.asarray(t, BF) for t in x_tables())
    outer_f, outer_b = jnp.asarray(z_outer(-1), BF), jnp.asarray(z_outer_back(), BF)
    inner_f, inner_b = jnp.asarray(z_inner(-1), BF), jnp.asarray(z_inner(1), BF)
    cw, sw = (jnp.asarray(t, F32) for t in twiddles())
    roll = pltpu.roll

    def exchange(x, axis):
        return lax.all_to_all(x, axis, split_axis=0, concat_axis=0, tiled=True, axis_index_groups=[ORDER[axis]])

    def s1(*a):
        return stage1(*a, roll)

    def s2(*a):
        return stage2(*a, roll)

    def s3(*a):
        return stage3(*a, lax.axis_index("row"), lax.axis_index("col"))

    def s4(*a):
        return stage4(*a, roll)

    def s5(*a):
        return stage5(*a, roll)

    flat = (ZL * YL, NX)
    x = call(s1, (G, 5, 4, LANES), pressure_rhs.reshape(flat), scalar_source.reshape(flat), fwd_x, fast=(False, True))
    x = exchange(x, "col")
    x = call(s2, (G, 4, 3 * LANES), x, outer_f, inner_f, cw, sw)
    x = exchange(x, "row")
    x = call(s3, (G, 4, 3 * LANES), x, forward_y, back_y, wall_rates.reshape(1, NY))
    x = exchange(x, "row")
    x = call(s4, (G, 5, 4, LANES), x, outer_b, inner_b, cw, sw)
    x = exchange(x, "col")
    outs = call(s5, [flat, flat], x, back_x, fast=(True, False))
    return tuple(o.reshape(ZL, YL, NX) for o in outs)


def solution(mesh):
    field = P("col", "row", None)
    return jax.shard_map(
        shards,
        mesh=mesh,
        in_specs=(field, field, P(), P(), P()),
        out_specs=(field, field),
        check_vma=False,
    )
```
